32 devices in a mesh: dp: 4 (over y, x), fsdp: 8 (over z, core).
Axes of the slice: x: 2, y: 2, z: 4, core: 2. Of those that a mesh axis runs over, the one named last changes fastest.
Arguments:
- text_in: bfloat16 [16384, 768], P(('dp', 'fsdp')), may hold values from -6 to 6
- layout_in: bfloat16 [16384, 192], P(('dp', 'fsdp')), may hold values from -6 to 6
- lengths: int32 [32], P(('dp', 'fsdp')), may hold values from 1 to 512, as said below
- attn_text: bfloat16 [768, 3072], P(None, ('dp', 'fsdp'))
- up_text: bfloat16 [768, 3072], P(None, ('dp', 'fsdp')), may hold values from -0.21875 to 0.21875
- down_text: bfloat16 [3072, 768], P(('dp', 'fsdp')), may hold values from -0.109375 to 0.109375
- attn_layout: bfloat16 [192, 768], P(None, ('dp', 'fsdp'))
- up_layout: bfloat16 [192, 768], P(None, ('dp', 'fsdp')), may hold values from -0.4375 to 0.4375
- down_layout: bfloat16 [768, 192], P(('dp', 'fsdp')), may hold values from -0.21875 to 0.21875
- norm_params: bfloat16 [3840], P(('dp', 'fsdp'))
- grad_text: bfloat16 [16384, 768], P(('dp', 'fsdp')), may hold values from -6 to 6
- grad_layout: bfloat16 [16384, 192], P(('dp', 'fsdp')), may hold values from -6 to 6
Outputs:
- text_out: bfloat16 [16384, 768], P(('dp', 'fsdp'))
- layout_out: bfloat16 [16384, 192], P(('dp', 'fsdp'))
- text_in_grad: bfloat16 [16384, 768], P(('dp', 'fsdp'))
- layout_in_grad: bfloat16 [16384, 192], P(('dp', 'fsdp'))
- attn_text_grad: float32 [768, 3072], P(None, ('dp', 'fsdp'))
- up_text_grad: float32 [768, 3072], P(None, ('dp', 'fsdp'))
- down_text_grad: float32 [3072, 768], P(('dp', 'fsdp'))
- attn_layout_grad: float32 [192, 768], P(None, ('dp', 'fsdp'))
- up_layout_grad: float32 [192, 768], P(None, ('dp', 'fsdp'))
- down_layout_grad: float32 [768, 192], P(('dp', 'fsdp'))
- norm_grad: float32 [3840], P(('dp', 'fsdp'))
The draws below stay inside these ranges and needn't reach their ends.
Inputs may be any that keep to these rules, and one draw needn't show every extreme that they name: Tokens held by each page slot; the first lengths[s] places of slot s are real tokens, the rest padding; at least one slot holds 512 tokens in every draw.
All inputs are finite; a program needn't handle non-finite values.
Results may differ from the reference program's by a relative error of at most 0.014.
Values may be sent and summed in bfloat16 or wider, within the bound.
A program may use at most 256 MiB of HBM per device.

```python
import jax
import jax.numpy as jnp
from jax import lax

D = 768
HEADS = 12
FF = 3072
DL = 192
FFL = 768
PAGE = 512
SLOTS = 32
ROWS = 16384


key_spread = 50.0


def packed_attention(key, model_width):
    values = jnp.clip(jax.random.normal(key, (model_width, 4 * model_width), jnp.float32), -5.0, 5.0)
    column = jnp.arange(4 * model_width)
    scale = jnp.where(column < 3 * model_width, model_width ** (-0.5), (key_spread / model_width) ** 0.5)
    return values * scale[None, :]


def draw_attn_text(key, part):
    return packed_attention(jax.random.fold_in(key, 11), D).astype(jnp.bfloat16)


def draw_attn_layout(key, part):
    return packed_attention(jax.random.fold_in(key, 13), DL).astype(jnp.bfloat16)


def draw_norm_params(key, part):
    total = 4 * D + 4 * DL
    index = jnp.arange(total)
    block = jnp.where(index < 4 * D, index // D, (index - 4 * D) // DL)
    is_gain = block % 2 == 0
    values = jnp.clip(jax.random.normal(jax.random.fold_in(key, 17), (total,), jnp.float32), -4.0, 4.0)
    return jnp.where(is_gain, 1.0 + 0.15 * values, 0.5 * values).astype(jnp.bfloat16)


def draw_lengths(key, part):
    first, second, third = jax.random.split(jax.random.fold_in(key, 19), 3)
    one_draw = jax.random.randint(first, (SLOTS,), 1, PAGE + 1)
    two_draw = jax.random.randint(second, (SLOTS,), 1, PAGE + 1)
    counts = jnp.maximum(one_draw, two_draw)
    chosen = jax.random.randint(third, (), 0, SLOTS)
    return jnp.where(jnp.arange(SLOTS) == chosen, PAGE, counts).astype(jnp.int32)


def raised(result, stream_key, source, target, parts, factor):
    def block_of(axis_at):
        return (jnp.arange(result.shape[axis_at]) // (result.shape[axis_at] // parts)).reshape((-1,) + (1,) * (result.ndim - 1 - axis_at))

    near = jax.random.permutation(stream_key, parts)[block_of(target)]
    second = (block_of(target) + parts // 2) % parts
    return jnp.where((block_of(source) == near) | (block_of(source) == second), factor * result, result)


def level_of(own_key, extent, cuts, smallest, high):
    factor_of, own = 1.0, jax.random.fold_in(own_key, 6)
    for position, parts in cuts:
        steps = jnp.exp(jax.random.uniform(jax.random.fold_in(own, position), (parts,), jnp.float32, smallest / len(cuts), high / len(cuts)))
        factor_of = factor_of * jnp.repeat(steps, extent[position] // parts).reshape([-1 if axis == position else 1 for axis in range(len(extent))])
    return factor_of


def bell_draw(rng, dims, deviation, reach, cuts=(), dtype=jnp.bfloat16):
    array = jax.random.normal(rng, dims, jnp.float32) * deviation
    if len(cuts) > 0:
        array = level_of(rng, dims, cuts, -0.22, 0.18) * array
    return jnp.clip(array, min=-reach, max=reach).astype(dtype)


def heavy_noise(stream_key, dims, width, bound, cuts, heavy, dtype=jnp.bfloat16):
    result = width * jax.random.normal(stream_key, dims, jnp.float32)
    if cuts:
        result = result * level_of(stream_key, dims, cuts, -0.22, 0.18)
    return jnp.clip(raised(result, jax.random.fold_in(stream_key, 3), *heavy), -bound, bound).astype(dtype)


def setup_inputs(seed: int = 0) -> dict:
    key_list = jax.random.split(jax.random.key(seed), 13)
    text_in = bell_draw(key_list[0], (ROWS, D), 1.0, 6.0, ((0, 32),))
    layout_in = bell_draw(key_list[1], (ROWS, DL), 1.0, 6.0, ((0, 32),))
    lengths = draw_lengths(jax.random.fold_in(key_list[12], 71), 0)
    attn_text = draw_attn_text(jax.random.fold_in(key_list[12], 71), 0)
    up_text = bell_draw(key_list[4], (D, FF), D ** -0.5, 0.21875, ((1, 32),))
    down_text = bell_draw(key_list[5], (FF, D), FF ** -0.5, 0.109375, ((0, 32),))
    attn_layout = draw_attn_layout(jax.random.fold_in(key_list[12], 71), 0)
    up_layout = bell_draw(key_list[7], (DL, FFL), DL ** -0.5, 0.4375, ((1, 32),))
    down_layout = bell_draw(key_list[8], (FFL, DL), FFL ** -0.5, 0.21875, ((0, 32),))
    norm_params = draw_norm_params(jax.random.fold_in(key_list[12], 71), 0)
    grad_text = heavy_noise(key_list[10], (ROWS, D), 1.0, 6.0, ((0, 32),), (0, 1, 32, 2.75))
    grad_layout = heavy_noise(key_list[11], (ROWS, DL), 1.0, 6.0, ((0, 32),), (0, 1, 32, 2.75))
    return {"text_in": text_in, "layout_in": layout_in, "lengths": lengths, "attn_text": attn_text, "up_text": up_text, "down_text": down_text, "attn_layout": attn_layout, "up_layout": up_layout, "down_layout": down_layout, "norm_params": norm_params, "grad_text": grad_text, "grad_layout": grad_layout}


@jax.custom_vjp
def low(v):
    return lax.optimization_barrier(v.astype(jnp.bfloat16)).astype(jnp.float32)

@jax.custom_vjp
def low_back(v):
    return v

def low_keep(v):
    return (low(v), None)

def low_pass(kept, grad):
    return (grad,)

def back_keep(v):
    return (v, None)

def back_low(kept, grad):
    return (low(grad),)
low.defvjp(low_keep, low_pass)
low_back.defvjp(back_keep, back_low)
EPSILON = 1e-05
NEG_FILL = -1000000000.0
HIGHEST = lax.Precision.HIGHEST

def matmul(left, right):
    return jnp.dot(left, right, precision=HIGHEST, preferred_element_type=jnp.float32)

def rounded(value):
    return low(low_back(value))

def layer_norm(hidden, gain, shift):
    centre = lax.optimization_barrier(jnp.mean(hidden, axis=-1, keepdims=True))
    centred = hidden - centre
    spread = lax.optimization_barrier(jnp.mean(centred * centred, axis=-1, keepdims=True))
    return centred * lax.rsqrt(spread + EPSILON) * gain + shift

def attend(pieces):
    query_text, key_text, value_text, query_layout, key_layout, value_layout, length = pieces
    raw_text = jnp.einsum('qhd,khd->hqk', query_text, key_text, precision=HIGHEST)
    raw_layout = jnp.einsum('qhd,khd->hqk', query_layout, key_layout, precision=HIGHEST)
    scores = low_back(raw_text) * query_text.shape[-1] ** (-0.5) + low_back(raw_layout) * query_layout.shape[-1] ** (-0.5)
    valid = jnp.arange(scores.shape[-1]) < length
    scores = jnp.where(valid[None, None, :], scores, NEG_FILL)
    row_top = lax.optimization_barrier(jnp.max(scores, axis=-1, keepdims=True))
    log_total = row_top + jnp.log(lax.optimization_barrier(jnp.sum(jnp.exp(scores - row_top), axis=-1, keepdims=True)))
    attn_probs = low(jnp.exp(scores - log_total))
    context_text = jnp.einsum('hqk,khd->qhd', attn_probs, value_text, precision=HIGHEST)
    context_layout = jnp.einsum('hqk,khd->qhd', attn_probs, value_layout, precision=HIGHEST)
    return (rounded(context_text), rounded(context_layout))

def project(stream_in, packed, model_width):
    slot_count = stream_in.shape[0] // PAGE
    projected = rounded(matmul(stream_in, packed[:, :3 * model_width]))
    shaped = projected.reshape(slot_count, PAGE, 3, HEADS, model_width // HEADS)
    return (shaped[:, :, 0], shaped[:, :, 1], shaped[:, :, 2])

def finish(stream_in, context, packed, up_weight, down_weight, norm_part, model_width):
    branch = low_back(matmul(context, packed[:, 3 * model_width:]))
    middle = layer_norm(stream_in + branch, norm_part[0], norm_part[1])
    inner = low_back(matmul(low(middle), up_weight))
    activated = low(jax.nn.gelu(inner, approximate=False))
    second = low_back(matmul(activated, down_weight))
    return layer_norm(middle + second, norm_part[2], norm_part[3])

def reference(text_in, layout_in, lengths, attn_text, up_text, down_text, attn_layout, up_layout, down_layout, norm_params, grad_text, grad_layout):

    def forward(text_f, layout_f, attn_tf, up_tf, down_tf, attn_lf, up_lf, down_lf, norm_f):
        query_text, key_text, value_text = project(text_f, attn_tf, D)
        query_layout, key_layout, value_layout = project(layout_f, attn_lf, DL)
        context_text, context_layout = lax.map(jax.checkpoint(attend), (query_text, key_text, value_text, query_layout, key_layout, value_layout, lengths))
        text_norms = norm_f[:4 * D].reshape(4, D)
        layout_norms = norm_f[4 * D:].reshape(4, DL)
        text_result = finish(text_f, context_text.reshape(-1, D), attn_tf, up_tf, down_tf, text_norms, D)
        layout_result = finish(layout_f, context_layout.reshape(-1, DL), attn_lf, up_lf, down_lf, layout_norms, DL)
        return (text_result, layout_result)
    outputs, backward = jax.vjp(forward, text_in.astype(jnp.float32), layout_in.astype(jnp.float32), attn_text.astype(jnp.float32), up_text.astype(jnp.float32), down_text.astype(jnp.float32), attn_layout.astype(jnp.float32), up_layout.astype(jnp.float32), down_layout.astype(jnp.float32), norm_params.astype(jnp.float32))
    grads = backward((grad_text.astype(jnp.float32), grad_layout.astype(jnp.float32)))
    return (outputs[0].astype(jnp.bfloat16), outputs[1].astype(jnp.bfloat16), grads[0].astype(jnp.bfloat16), grads[1].astype(jnp.bfloat16), grads[2], grads[3], grads[4], grads[5], grads[6], grads[7], grads[8])
```

```python
import functools

import jax
import jax.numpy as jnp
from jax import lax
from jax.experimental import pallas as pl
from jax.experimental.pallas import tpu as pltpu
from jax.sharding import PartitionSpec as P

HEADS = 12
EPSILON = 1e-05
NEG_FILL = -1000000000.0
AXES = ("dp", "fsdp")
BF16 = jnp.bfloat16
F32 = jnp.float32
ROW_STEP = 64


def mm(a, b, dim_a, dim_b):
    return lax.dot_general(a, b, (((dim_a,), (dim_b,)), ((), ())), preferred_element_type=F32)


def loop(count, body):
    def step(i, carry):
        body(i)
        return carry

    lax.fori_loop(0, count, step, 0)


def steps(total, size):
    size = min(size, total)
    assert total % size == 0
    return total // size, size


def at(i, size):
    return pl.ds(pl.multiple_of(i * size, size), size)


def project_heads(x, weight, qkv, scale, chunk):
    width = x.shape[1]
    count, size = steps(width, chunk)

    def body(i):
        block = mm(weight[at(i, size), :], x[...], 1, 1).astype(BF16).astype(F32)
        qkv[at(i, size), :] = (block * jnp.where(i < count, scale, 1.0)).astype(BF16)

    loop(3 * count, body)


def head_rows(ref, part, head, dim, width):
    return ref[pl.ds(pl.multiple_of(part * width + head * dim, dim), dim), :]


def joined(text_ref, layout_ref, part, head, dims, widths):
    return jnp.concatenate(
        [
            head_rows(text_ref, part, head, dims[0], widths[0]),
            head_rows(layout_ref, part, head, dims[1], widths[1]),
        ],
        axis=0,
    )


def masked_scores(query, key, length):
    scores = mm(key, query, 0, 0)
    place = lax.broadcasted_iota(jnp.int32, scores.shape, 0)
    return jnp.where(place < length, scores, NEG_FILL)


def attend_head(head, length, qkv_t, qkv_l, ctx_t, ctx_l, lse, dims, widths):
    query = joined(qkv_t, qkv_l, 0, head, dims, widths)
    key = joined(qkv_t, qkv_l, 1, head, dims, widths)
    value = joined(qkv_t, qkv_l, 2, head, dims, widths)
    scores = masked_scores(query, key, length)
    top = jnp.max(scores, axis=0, keepdims=True)
    grown = jnp.exp(scores - top)
    total = jnp.sum(grown, axis=0, keepdims=True)
    lse[head] = top + jnp.log(total)
    context = mm(value, grown.astype(BF16), 1, 0) * (1.0 / total)
    ctx_t[pl.ds(pl.multiple_of(head * dims[0], dims[0]), dims[0]), :] = context[: dims[0]].astype(BF16)
    ctx_l[pl.ds(pl.multiple_of(head * dims[1], dims[1]), dims[1]), :] = context[dims[0] :].astype(BF16)


def attend_head_back(
    head, length, qkv_t, qkv_l, dctx_t, dctx_l, lse, dqkv_t, dqkv_l, dims, widths, scales
):
    query = joined(qkv_t, qkv_l, 0, head, dims, widths)
    key = joined(qkv_t, qkv_l, 1, head, dims, widths)
    value = joined(qkv_t, qkv_l, 2, head, dims, widths)
    dcontext = joined(dctx_t, dctx_l, 0, head, dims, widths)
    scores = masked_scores(query, key, length)
    probs = jnp.exp(scores - lse[head])
    dvalue = mm(dcontext, probs.astype(BF16), 1, 1)
    dprobs = mm(value, dcontext, 0, 0)
    inner = jnp.sum(dprobs * probs, axis=0, keepdims=True)
    dscores = (probs * (dprobs - inner)).astype(BF16)
    dkey = mm(query, dscores, 1, 1)
    dquery = mm(key, dscores, 1, 0)
    for part, grad in ((0, dquery), (1, dkey), (2, dvalue)):
        for ref, dim, width, scale, rows in (
            (dqkv_t, dims[0], widths[0], scales[0], grad[: dims[0]]),
            (dqkv_l, dims[1], widths[1], scales[1], grad[dims[0] :]),
        ):
            rows = rows * scale if part == 0 else rows
            ref[pl.ds(pl.multiple_of(part * width + head * dim, dim), dim), :] = rows.astype(BF16)


def normed(hidden):
    centred = hidden - jnp.mean(hidden, axis=-1, keepdims=True)
    rate = lax.rsqrt(jnp.mean(centred * centred, axis=-1, keepdims=True) + EPSILON)
    return centred * rate, rate


def norm_back(grad, hat, rate, gain):
    scaled = grad * gain
    mean = jnp.mean(scaled, axis=-1, keepdims=True)
    along = jnp.mean(scaled * hat, axis=-1, keepdims=True)
    return rate * (scaled - mean - hat * along)


def column_sum(values):
    return jnp.sum(values, axis=0, keepdims=True)


def stream_first(x, ctx_tr, ctx, weight, norms, acc, hat, rate, low):
    rows, width = x.shape
    ctx[...] = ctx_tr[...].T
    count, size = steps(rows, 256)

    def product(i):
        acc[at(i, size), :] = mm(ctx[at(i, size), :], weight[3 * width : 4 * width, :], 1, 1)

    loop(count, product)

    def norm(i):
        block = at(i, ROW_STEP)
        hat_b, rate_b = normed(x[block, :].astype(F32) + acc[block, :])
        hat[block, :] = hat_b
        rate[block, :] = rate_b
        low[block, :] = (hat_b * norms[0:1, :] + norms[1:2, :]).astype(BF16)

    loop(rows // ROW_STEP, norm)


def stream_inner(low, up, down, act, slope, acc, chunk):
    count, size = steps(up.shape[0], chunk)
    acc[...] = jnp.zeros_like(acc)

    def body(i):
        block = at(i, size)
        inner = mm(up[block, :], low[...], 1, 1)
        cdf = 0.5 + 0.5 * lax.erf(inner * (0.5**0.5))
        density = jnp.exp(inner * inner * -0.5) * (0.5 / jnp.pi) ** 0.5
        act[block, :] = (inner * cdf).astype(BF16)
        slope[block, :] = (cdf + inner * density).astype(BF16)
        acc[...] += mm(act[block, :], down[block, :], 0, 0)

    loop(count, body)


def stream_second(g, norms, acc, hat, out, dhid, dlow, gnorm):
    rows, width = g.shape

    def body(i, sums):
        block = at(i, ROW_STEP)
        hidden = hat[block, :] * norms[0:1, :] + norms[1:2, :] + acc[block, :]
        hat_b, rate_b = normed(hidden)
        out[block, :] = (hat_b * norms[2:3, :] + norms[3:4, :]).astype(BF16)
        grad = g[block, :].astype(F32)
        back = norm_back(grad, hat_b, rate_b, norms[2:3, :])
        dhid[block, :] = back
        dlow[block, :] = back.astype(BF16)
        return sums[0] + column_sum(grad * hat_b), sums[1] + column_sum(grad)

    zero = jnp.zeros((1, width), F32)
    sums = lax.fori_loop(0, rows // ROW_STEP, body, (zero, zero))
    gnorm[2:3, :] = sums[0]
    gnorm[3:4, :] = sums[1]


def stream_inner_back(low, dlow, up, down, act, slope, dhid, gup, gdown, chunk, done):
    count, size = steps(up.shape[0], chunk)

    def body(i):
        block = at(i, size)
        dact = mm(down[block, :], dlow[...], 1, 1)
        dinner = (dact * slope[block, :].astype(F32)).astype(BF16)
        dhid[...] += mm(dinner, up[block, :], 0, 0)
        gdown[block, :] = mm(act[block, :], dlow[...], 1, 0).astype(gdown.dtype)
        gup[block, :] = mm(dinner, low[...], 1, 0).astype(gup.dtype)
        done(i, block)

    loop(count, body)
    return count


def stream_first_back(norms, hat, rate, dhid, dlow, ctx, weight, dctx, gattn, gnorm):
    rows, width = hat.shape

    def body(i, sums):
        block = at(i, ROW_STEP)
        grad = dhid[block, :]
        hat_b = hat[block, :]
        back = norm_back(grad, hat_b, rate[block, :], norms[0:1, :])
        dhid[block, :] = back
        dlow[block, :] = back.astype(BF16)
        return sums[0] + column_sum(grad * hat_b), sums[1] + column_sum(grad)

    zero = jnp.zeros((1, width), F32)
    sums = lax.fori_loop(0, rows // ROW_STEP, body, (zero, zero))
    gnorm[0:1, :] = sums[0]
    gnorm[1:2, :] = sums[1]
    dctx[...] = mm(dlow[...], weight[3 * width : 4 * width, :], 1, 0).astype(BF16).T
    gattn[3 * width : 4 * width, :] = mm(dlow[...], ctx[...], 0, 0).astype(gattn.dtype)


def project_back(x, weight, dqkv, dhid, dx, gattn, chunk, done):
    width = x.shape[1]
    count, size = steps(3 * width, chunk)

    def body(i):
        block = at(i, size)
        dhid[...] += mm(dqkv[block, :], weight[block, :], 0, 0)
        gattn[block, :] = mm(dqkv[block, :], x[...], 1, 0).astype(gattn.dtype)
        done(i, block)

    loop(count, body)
    loop(x.shape[0] // ROW_STEP, lambda i: store_low(dx, dhid, at(i, ROW_STEP)))
    return count


def store_low(out, values, block):
    out[block, :] = values[block, :].astype(BF16)


def layer_kernel(dims, scales, chunks, *refs):
    (
        lengths, x, y, gx, gy, tnorm, lnorm, hattn, hup, hdown, lattn, lup, ldown,
        text_out, layout_out, dx, dy, oattn, oup, odown, glattn, glup, gldown, gtnorm, glnorm,
        attn, up, down, qkv_t, qkv_l, dqkv_t, dqkv_l, ctx_tt, ctx_tl, ctx_t, ctx_l, dctx_t, dctx_l,
        act_t, act_l, slope_t, slope_l, acc_t, acc_l, hat_t, hat_l, dhid_t, dhid_l,
        low_t, low_l, dlow_t, dlow_l, rate_t, rate_l, lse, in_sem, out_sem,
    ) = refs
    widths = (x.shape[1], y.shape[1])
    length = lengths[0]
    loads = [
        pltpu.make_async_copy(src, dst, in_sem.at[i])
        for i, (src, dst) in enumerate(((hattn, attn), (hup, up), (hdown, down)))
    ]
    for load in loads:
        load.start()
    project_heads(y, lattn, qkv_l, scales[1], chunks[1])
    loads[0].wait()
    project_heads(x, attn, qkv_t, scales[0], chunks[0])
    loop(
        HEADS,
        lambda h: attend_head(h, length, qkv_t, qkv_l, ctx_tt, ctx_tl, lse, dims, widths),
    )
    loads[1].wait()
    loads[2].wait()
    nothing = lambda i, block: None
    stream_first(y, ctx_tl, ctx_l, lattn, lnorm, acc_l, hat_l, rate_l, low_l)
    stream_inner(low_l, lup, ldown, act_l, slope_l, acc_l, chunks[1])
    stream_second(gy, lnorm, acc_l, hat_l, layout_out, dhid_l, dlow_l, glnorm)
    stream_inner_back(
        low_l, dlow_l, lup, ldown, act_l, slope_l, dhid_l, glup, gldown, chunks[1], nothing
    )
    stream_first_back(lnorm, hat_l, rate_l, dhid_l, dlow_l, ctx_l, lattn, dctx_l, glattn, glnorm)

    def send(source, target, block):
        pltpu.make_async_copy(source.at[block, :], target.at[block, :], out_sem).start()

    def sent_inner(i, block):
        send(up, oup, block)
        send(down, odown, block)

    stream_first(x, ctx_tt, ctx_t, attn, tnorm, acc_t, hat_t, rate_t, low_t)
    stream_inner(low_t, up, down, act_t, slope_t, acc_t, chunks[0])
    stream_second(gx, tnorm, acc_t, hat_t, text_out, dhid_t, dlow_t, gtnorm)
    stream_inner_back(
        low_t, dlow_t, up, down, act_t, slope_t, dhid_t, up, down, chunks[0], sent_inner
    )
    stream_first_back(tnorm, hat_t, rate_t, dhid_t, dlow_t, ctx_t, attn, dctx_t, attn, gtnorm)
    loop(
        HEADS,
        lambda h: attend_head_back(
            h, length, qkv_t, qkv_l, dctx_t, dctx_l, lse, dqkv_t, dqkv_l, dims, widths, scales
        ),
    )
    project_back(y, lattn, dqkv_l, dhid_l, dy, glattn, chunks[1], nothing)
    width = widths[0]
    send(attn, oattn, pl.ds(3 * width, width))
    project_back(
        x, attn, dqkv_t, dhid_t, dx, attn, chunks[0], lambda i, block: send(attn, oattn, block)
    )
    for source, target in ((up, oup), (down, odown), (attn, oattn)):
        pltpu.make_async_copy(source, target, out_sem).wait()


def layer(x, y, lengths, gx, gy, tnorm, lnorm, attn, up, down, lattn, lup, ldown):
    rows, width = x.shape
    lwidth = y.shape[1]
    inner, linner = up.shape[0], lup.shape[0]
    dims = (width // HEADS, lwidth // HEADS)
    scales = tuple(float(dim) ** -0.5 for dim in dims)
    vmem = pl.BlockSpec(memory_space=pltpu.VMEM)
    anywhere = pl.BlockSpec(memory_space=pl.ANY)
    smem = pl.BlockSpec(memory_space=pltpu.SMEM)
    like = jax.ShapeDtypeStruct

    def both(shape_of, dtype):
        return [pltpu.VMEM(shape_of(width, inner), dtype), pltpu.VMEM(shape_of(lwidth, linner), dtype)]

    scratch = [
        pltpu.VMEM(attn.shape, BF16),
        pltpu.VMEM(up.shape, BF16),
        pltpu.VMEM(down.shape, BF16),
        *both(lambda w, f: (3 * w, rows), BF16),
        *both(lambda w, f: (3 * w, rows), BF16),
        *both(lambda w, f: (w, rows), BF16),
        *both(lambda w, f: (rows, w), BF16),
        *both(lambda w, f: (w, rows), BF16),
        *both(lambda w, f: (f, rows), BF16),
        *both(lambda w, f: (f, rows), BF16),
        *both(lambda w, f: (rows, w), F32),
        *both(lambda w, f: (rows, w), F32),
        *both(lambda w, f: (rows, w), F32),
        *both(lambda w, f: (rows, w), BF16),
        *both(lambda w, f: (rows, w), BF16),
        *both(lambda w, f: (rows, 1), F32),
        pltpu.VMEM((HEADS, 1, rows), F32),
        pltpu.SemaphoreType.DMA((3,)),
        pltpu.SemaphoreType.DMA,
    ]
    return pl.pallas_call(
        functools.partial(layer_kernel, dims, scales, (384, 192)),
        out_shape=[
            like(x.shape, BF16),
            like(y.shape, BF16),
            like(x.shape, BF16),
            like(y.shape, BF16),
            like(attn.shape, BF16),
            like(up.shape, BF16),
            like(down.shape, BF16),
            like(lattn.shape, F32),
            like(lup.shape, F32),
            like(ldown.shape, F32),
            like(tnorm.shape, F32),
            like(lnorm.shape, F32),
        ],
        in_specs=[smem] + [vmem] * 6 + [anywhere] * 3 + [vmem] * 3,
        out_specs=[vmem] * 4 + [anywhere] * 3 + [vmem] * 5,
        scratch_shapes=scratch,
        compiler_params=pltpu.CompilerParams(vmem_limit_bytes=67043328),
        name="layer",
    )(lengths, x, y, gx, gy, tnorm, lnorm, attn, up, down, lattn, lup, ldown)


def per_device(
    text_in, layout_in, lengths, attn_text, up_text, down_text,
    attn_layout, up_layout, down_layout, norm_params, grad_text, grad_layout,
):
    width, lwidth = text_in.shape[1], layout_in.shape[1]
    owners = lax.axis_size(AXES)
    part = down_layout.shape[0]
    count = norm_params.shape[0]

    def gather(piece):
        return lax.all_gather(piece, AXES, axis=0, tiled=True)

    attn, up, down = gather(attn_text.T), gather(up_text.T), gather(down_text)
    norm_row = jnp.pad(norm_params, (0, -count % lwidth)).reshape(-1, lwidth)
    small = gather(jnp.concatenate([attn_layout.T, up_layout.T, down_layout, norm_row], axis=0))
    nrows = norm_row.shape[0]
    small = small.reshape(owners, 3 * part + nrows, lwidth)
    lattn, lup, ldown = (
        small[:, i * part : (i + 1) * part].reshape(owners * part, lwidth) for i in range(3)
    )
    norms = small[:, 3 * part :].reshape(owners, -1)[:, :count].reshape(-1).astype(F32)
    tnorm = norms[: 4 * width].reshape(4, width)
    lnorm = norms[4 * width :].reshape(4, lwidth)
    (
        text_out, layout_out, dx, dy, gattn, gup, gdown, glattn, glup, gldown, gtnorm, glnorm,
    ) = layer(
        text_in, layout_in, lengths, grad_text, grad_layout, tnorm, lnorm,
        attn, up, down, lattn, lup, ldown,
    )

    def scatter(piece):
        return lax.psum_scatter(piece, AXES, scatter_dimension=0, tiled=True)

    gnorm = jnp.concatenate([gtnorm.reshape(-1), glnorm.reshape(-1)]).reshape(owners, count)
    gsmall = jnp.concatenate(
        [piece.reshape(owners, part, lwidth) for piece in (glattn, glup, gldown)]
        + [jnp.pad(gnorm, ((0, 0), (0, -count % lwidth))).reshape(owners, nrows, lwidth)],
        axis=1,
    )
    gsmall = scatter(gsmall.reshape(-1, lwidth))
    gattn, gup, gdown = (scatter(piece).astype(F32) for piece in (gattn, gup, gdown))
    return (
        text_out,
        layout_out,
        dx,
        dy,
        gattn.T,
        gup.T,
        gdown,
        gsmall[:part].T,
        gsmall[part : 2 * part].T,
        gsmall[2 * part : 3 * part],
        gsmall[3 * part :].reshape(-1)[:count],
    )


def solution(mesh):
    rows, columns = P(AXES, None), P(None, AXES)
    split = P(AXES)
    return jax.shard_map(
        per_device,
        mesh=mesh,
        in_specs=(
            rows, rows, split, columns, columns, rows, columns, columns, rows, split, rows, rows,
        ),
        out_specs=(rows, rows, rows, rows, columns, columns, rows, columns, columns, rows, split),
        check_vma=False,
    )
```

```python
import functools

import jax
import jax.numpy as jnp
from jax import lax
from jax.experimental import pallas as pl
from jax.experimental.pallas import tpu as pltpu
from jax.sharding import PartitionSpec as P

HEADS = 12
EPSILON = 1e-05
NEG_FILL = -1000000000.0
AXES = ("dp", "fsdp")
BF16 = jnp.bfloat16
F32 = jnp.float32
ROW_STEP = 64


def mm(a, b, dim_a, dim_b):
    return lax.dot_general(a, b, (((dim_a,), (dim_b,)), ((), ())), preferred_element_type=F32)


def loop(count, body):
    def step(i, carry):
        body(i)
        return carry

    lax.fori_loop(0, count, step, 0)


def steps(total, size):
    size = min(size, total)
    assert total % size == 0
    return total // size, size


def at(i, size):
    return pl.ds(pl.multiple_of(i * size, size), size)


def project_heads(x, weight, qkv, scale, chunk):
    width = x.shape[1]
    count, size = steps(width, chunk)

    def body(i):
        block = mm(weight[at(i, size), :], x[...], 1, 1).astype(BF16).astype(F32)
        qkv[at(i, size), :] = (block * jnp.where(i < count, scale, 1.0)).astype(BF16)

    loop(3 * count, body)


def head_rows(ref, part, head, dim, width):
    return ref[pl.ds(pl.multiple_of(part * width + head * dim, dim), dim), :]


def joined(text_ref, layout_ref, part, head, dims, widths):
    return jnp.concatenate(
        [
            head_rows(text_ref, part, head, dims[0], widths[0]),
            head_rows(layout_ref, part, head, dims[1], widths[1]),
        ],
        axis=0,
    )


def masked_scores(query, key, length):
    scores = mm(key, query, 0, 0)
    place = lax.broadcasted_iota(jnp.int32, scores.shape, 0)
    return jnp.where(place < length, scores, NEG_FILL)


def attend_head(head, length, qkv_t, qkv_l, ctx_t, ctx_l, lse, dims, widths):
    query = joined(qkv_t, qkv_l, 0, head, dims, widths)
    key = joined(qkv_t, qkv_l, 1, head, dims, widths)
    value = joined(qkv_t, qkv_l, 2, head, dims, widths)
    scores = masked_scores(query, key, length)
    top = jnp.max(scores, axis=0, keepdims=True)
    grown = jnp.exp(scores - top)
    total = jnp.sum(grown, axis=0, keepdims=True)
    lse[head] = top + jnp.log(total)
    context = mm(value, grown.astype(BF16), 1, 0) * (1.0 / total)
    ctx_t[pl.ds(pl.multiple_of(head * dims[0], dims[0]), dims[0]), :] = context[: dims[0]].astype(BF16)
    ctx_l[pl.ds(pl.multiple_of(head * dims[1], dims[1]), dims[1]), :] = context[dims[0] :].astype(BF16)


def attend_head_back(
    head, length, qkv_t, qkv_l, dctx_t, dctx_l, lse, dqkv_t, dqkv_l, dims, widths, scales
):
    query = joined(qkv_t, qkv_l, 0, head, dims, widths)
    key = joined(qkv_t, qkv_l, 1, head, dims, widths)
    value = joined(qkv_t, qkv_l, 2, head, dims, widths)
    dcontext = joined(dctx_t, dctx_l, 0, head, dims, widths)
    scores = masked_scores(query, key, length)
    probs = jnp.exp(scores - lse[head])
    dvalue = mm(dcontext, probs.astype(BF16), 1, 1)
    dprobs = mm(value, dcontext, 0, 0)
    inner = jnp.sum(dprobs * probs, axis=0, keepdims=True)
    dscores = (probs * (dprobs - inner)).astype(BF16)
    dkey = mm(query, dscores, 1, 1)
    dquery = mm(key, dscores, 1, 0)
    for part, grad in ((0, dquery), (1, dkey), (2, dvalue)):
        for ref, dim, width, scale, rows in (
            (dqkv_t, dims[0], widths[0], scales[0], grad[: dims[0]]),
            (dqkv_l, dims[1], widths[1], scales[1], grad[dims[0] :]),
        ):
            rows = rows * scale if part == 0 else rows
            ref[pl.ds(pl.multiple_of(part * width + head * dim, dim), dim), :] = rows.astype(BF16)


def normed(hidden):
    centred = hidden - jnp.mean(hidden, axis=-1, keepdims=True)
    rate = lax.rsqrt(jnp.mean(centred * centred, axis=-1, keepdims=True) + EPSILON)
    return centred * rate, rate


def norm_back(grad, hat, rate, gain):
    scaled = grad * gain
    mean = jnp.mean(scaled, axis=-1, keepdims=True)
    along = jnp.mean(scaled * hat, axis=-1, keepdims=True)
    return rate * (scaled - mean - hat * along)


def column_sum(values):
    return jnp.sum(values, axis=0, keepdims=True)


def stream_first(x, ctx_tr, ctx, weight, norms, acc, hat, rate, low):
    rows, width = x.shape
    ctx[...] = ctx_tr[...].T
    count, size = steps(rows, 256)

    def product(i):
        acc[at(i, size), :] = mm(ctx[at(i, size), :], weight[3 * width : 4 * width, :], 1, 1)

    loop(count, product)

    def norm(i):
        block = at(i, ROW_STEP)
        hat_b, rate_b = normed(x[block, :].astype(F32) + acc[block, :])
        hat[block, :] = hat_b
        rate[block, :] = rate_b
        low[block, :] = (hat_b * norms[0:1, :] + norms[1:2, :]).astype(BF16)

    loop(rows // ROW_STEP, norm)


def stream_inner(low, up, down, act, slope, acc, chunk):
    count, size = steps(up.shape[0], chunk)
    acc[...] = jnp.zeros_like(acc)

    def body(i):
        block = at(i, size)
        inner = mm(up[block, :], low[...], 1, 1)
        cdf = 0.5 + 0.5 * lax.erf(inner * (0.5**0.5))
        density = jnp.exp(inner * inner * -0.5) * (0.5 / jnp.pi) ** 0.5
        act[block, :] = (inner * cdf).astype(BF16)
        slope[block, :] = (cdf + inner * density).astype(BF16)
        acc[...] += mm(act[block, :], down[block, :], 0, 0)

    loop(count, body)


def stream_second(g, norms, acc, hat, out, dhid, dlow, gnorm):
    rows, width = g.shape

    def body(i, sums):
        block = at(i, ROW_STEP)
        hidden = hat[block, :] * norms[0:1, :] + norms[1:2, :] + acc[block, :]
        hat_b, rate_b = normed(hidden)
        out[block, :] = (hat_b * norms[2:3, :] + norms[3:4, :]).astype(BF16)
        grad = g[block, :].astype(F32)
        back = norm_back(grad, hat_b, rate_b, norms[2:3, :])
        dhid[block, :] = back
        dlow[block, :] = back.astype(BF16)
        return sums[0] + column_sum(grad * hat_b), sums[1] + column_sum(grad)

    zero = jnp.zeros((1, width), F32)
    sums = lax.fori_loop(0, rows // ROW_STEP, body, (zero, zero))
    gnorm[2:3, :] = sums[0]
    gnorm[3:4, :] = sums[1]


def stream_inner_back(low, dlow, up, down, act, slope, dhid, gup, gdown, chunk, done):
    count, size = steps(up.shape[0], chunk)

    def body(i):
        block = at(i, size)
        dact = mm(down[block, :], dlow[...], 1, 1)
        dinner = (dact * slope[block, :].astype(F32)).astype(BF16)
        dhid[...] += mm(dinner, up[block, :], 0, 0)
        gdown[block, :] = mm(act[block, :], dlow[...], 1, 0).astype(gdown.dtype)
        gup[block, :] = mm(dinner, low[...], 1, 0).astype(gup.dtype)
        done(i, block)

    loop(count, body)
    return count


def stream_first_back(norms, hat, rate, dhid, dlow, ctx, weight, dctx, gattn, gnorm):
    rows, width = hat.shape

    def body(i, sums):
        block = at(i, ROW_STEP)
        grad = dhid[block, :]
        hat_b = hat[block, :]
        back = norm_back(grad, hat_b, rate[block, :], norms[0:1, :])
        dhid[block, :] = back
        dlow[block, :] = back.astype(BF16)
        return sums[0] + column_sum(grad * hat_b), sums[1] + column_sum(grad)

    zero = jnp.zeros((1, width), F32)
    sums = lax.fori_loop(0, rows // ROW_STEP, body, (zero, zero))
    gnorm[0:1, :] = sums[0]
    gnorm[1:2, :] = sums[1]
    dctx[...] = mm(dlow[...], weight[3 * width : 4 * width, :], 1, 0).astype(BF16).T
    gattn[3 * width : 4 * width, :] = mm(dlow[...], ctx[...], 0, 0).astype(gattn.dtype)


def project_back(x, weight, dqkv, dhid, dx, gattn, chunk, done):
    width = x.shape[1]
    count, size = steps(3 * width, chunk)

    def body(i):
        block = at(i, size)
        dhid[...] += mm(dqkv[block, :], weight[block, :], 0, 0)
        gattn[block, :] = mm(dqkv[block, :], x[...], 1, 0).astype(gattn.dtype)
        done(i, block)

    loop(count, body)
    loop(x.shape[0] // ROW_STEP, lambda i: store_low(dx, dhid, at(i, ROW_STEP)))
    return count


def store_low(out, values, block):
    out[block, :] = values[block, :].astype(BF16)


def layer_kernel(dims, scales, chunks, *refs):
    (
        lengths, x, y, gx, gy, tnorm, lnorm, hattn, hup, hdown, lattn, lup, ldown,
        text_out, layout_out, dx, dy, oattn, oup, odown, glattn, glup, gldown, gtnorm, glnorm,
        attn, up, down, qkv_t, qkv_l, dqkv_t, dqkv_l, ctx_tt, ctx_tl, ctx_t, ctx_l, dctx_t, dctx_l,
        act_t, act_l, slope_t, slope_l, acc_t, acc_l, hat_t, hat_l, dhid_t, dhid_l,
        low_t, low_l, dlow_t, dlow_l, rate_t, rate_l, lse, in_sem, out_sem,
    ) = refs
    widths = (x.shape[1], y.shape[1])
    length = lengths[0]
    loads = [
        pltpu.make_async_copy(src, dst, in_sem.at[i])
        for i, (src, dst) in enumerate(((hattn, attn), (hup, up), (hdown, down)))
    ]
    for load in loads:
        load.start()
    project_heads(y, lattn, qkv_l, scales[1], chunks[1])
    loads[0].wait()
    project_heads(x, attn, qkv_t, scales[0], chunks[0])
    loop(
        HEADS,
        lambda h: attend_head(h, length, qkv_t, qkv_l, ctx_tt, ctx_tl, lse, dims, widths),
    )
    loads[1].wait()
    loads[2].wait()
    nothing = lambda i, block: None
    stream_first(y, ctx_tl, ctx_l, lattn, lnorm, acc_l, hat_l, rate_l, low_l)
    stream_inner(low_l, lup, ldown, act_l, slope_l, acc_l, chunks[1])
    stream_second(gy, lnorm, acc_l, hat_l, layout_out, dhid_l, dlow_l, glnorm)
    stream_inner_back(
        low_l, dlow_l, lup, ldown, act_l, slope_l, dhid_l, glup, gldown, chunks[1], nothing
    )
    stream_first_back(lnorm, hat_l, rate_l, dhid_l, dlow_l, ctx_l, lattn, dctx_l, glattn, glnorm)

    def send(source, target, block):
        pltpu.make_async_copy(source.at[block, :], target.at[block, :], out_sem).start()

    def sent_inner(i, block):
        send(up, oup, block)
        send(down, odown, block)

    stream_first(x, ctx_tt, ctx_t, attn, tnorm, acc_t, hat_t, rate_t, low_t)
    stream_inner(low_t, up, down, act_t, slope_t, acc_t, chunks[0])
    stream_second(gx, tnorm, acc_t, hat_t, text_out, dhid_t, dlow_t, gtnorm)
    stream_inner_back(
        low_t, dlow_t, up, down, act_t, slope_t, dhid_t, up, down, chunks[0], sent_inner
    )
    stream_first_back(tnorm, hat_t, rate_t, dhid_t, dlow_t, ctx_t, attn, dctx_t, attn, gtnorm)
    loop(
        HEADS,
        lambda h: attend_head_back(
            h, length, qkv_t, qkv_l, dctx_t, dctx_l, lse, dqkv_t, dqkv_l, dims, widths, scales
        ),
    )
    project_back(y, lattn, dqkv_l, dhid_l, dy, glattn, chunks[1], nothing)
    width = widths[0]
    send(attn, oattn, pl.ds(3 * width, width))
    project_back(
        x, attn, dqkv_t, dhid_t, dx, attn, chunks[0], lambda i, block: send(attn, oattn, block)
    )
    for source, target in ((up, oup), (down, odown), (attn, oattn)):
        pltpu.make_async_copy(source, target, out_sem).wait()


def layer(x, y, lengths, gx, gy, tnorm, lnorm, attn, up, down, lattn, lup, ldown):
    rows, width = x.shape
    lwidth = y.shape[1]
    inner, linner = up.shape[0], lup.shape[0]
    dims = (width // HEADS, lwidth // HEADS)
    scales = tuple(float(dim) ** -0.5 for dim in dims)
    vmem = pl.BlockSpec(memory_space=pltpu.VMEM)
    anywhere = pl.BlockSpec(memory_space=pl.ANY)
    smem = pl.BlockSpec(memory_space=pltpu.SMEM)
    like = jax.ShapeDtypeStruct

    def both(shape_of, dtype):
        return [pltpu.VMEM(shape_of(width, inner), dtype), pltpu.VMEM(shape_of(lwidth, linner), dtype)]

    scratch = [
        pltpu.VMEM(attn.shape, BF16),
        pltpu.VMEM(up.shape, BF16),
        pltpu.VMEM(down.shape, BF16),
        *both(lambda w, f: (3 * w, rows), BF16),
        *both(lambda w, f: (3 * w, rows), BF16),
        *both(lambda w, f: (w, rows), BF16),
        *both(lambda w, f: (rows, w), BF16),
        *both(lambda w, f: (w, rows), BF16),
        *both(lambda w, f: (f, rows), BF16),
        *both(lambda w, f: (f, rows), BF16),
        *both(lambda w, f: (rows, w), F32),
        *both(lambda w, f: (rows, w), F32),
        *both(lambda w, f: (rows, w), F32),
        *both(lambda w, f: (rows, w), BF16),
        *both(lambda w, f: (rows, w), BF16),
        *both(lambda w, f: (rows, 1), F32),
        pltpu.VMEM((HEADS, 1, rows), F32),
        pltpu.SemaphoreType.DMA((3,)),
        pltpu.SemaphoreType.DMA,
    ]
    return pl.pallas_call(
        functools.partial(layer_kernel, dims, scales, (384, 192)),
        out_shape=[
            like(x.shape, BF16),
            like(y.shape, BF16),
            like(x.shape, BF16),
            like(y.shape, BF16),
            like(attn.shape, BF16),
            like(up.shape, BF16),
            like(down.shape, BF16),
            like(lattn.shape, F32),
            like(lup.shape, F32),
            like(ldown.shape, F32),
            like(tnorm.shape, F32),
            like(lnorm.shape, F32),
        ],
        in_specs=[smem] + [vmem] * 6 + [anywhere] * 3 + [vmem] * 3,
        out_specs=[vmem] * 4 + [anywhere] * 3 + [vmem] * 5,
        scratch_shapes=scratch,
        compiler_params=pltpu.CompilerParams(vmem_limit_bytes=67043328),
        name="layer",
    )(lengths, x, y, gx, gy, tnorm, lnorm, attn, up, down, lattn, lup, ldown)


def coordinates(planes):
    pair, column = lax.axis_index("dp"), lax.axis_index("fsdp")
    x, y = lax.rem(pair, 2), pair // 2
    plane, core = column // 2, lax.rem(column, 2)
    across = (pair + 1 - 2 * x, pair + 2 - 4 * y)
    return pair, plane, core, across


def entry_barrier(planes):
    pair, plane, core, across = coordinates(planes)
    barrier = pltpu.get_barrier_semaphore()

    def greet(target_pair, target_plane, target_core):
        pl.semaphore_signal(
            barrier,
            inc=1,
            device_id=(target_pair, target_plane * 2 + target_core),
            device_id_type=pl.DeviceIdType.MESH,
        )

    greet(across[0], plane, core)
    greet(across[1], plane, core)
    greet(pair, plane, 1 - core)
    pl.when(plane > 0)(lambda: greet(pair, plane - 1, core))
    pl.when(plane < planes - 1)(lambda: greet(pair, plane + 1, core))
    edges = jnp.where(plane > 0, 1, 0) + jnp.where(plane < planes - 1, 1, 0)
    pl.semaphore_wait(barrier, 3 + edges)


class Gather:
    def __init__(self, planes, units, send_sem, recv_sem):
        self.planes, self.units = planes, units
        self.send_sem, self.recv_sem = send_sem, recv_sem
        self.pair, self.plane, self.core, self.across = coordinates(planes)

    def block(self, unit, pair, plane, core):
        _, whole, before, after, _ = self.units[unit]
        return whole.at[(*before, pair, plane, core, *after)]

    def copy(self, unit, block, slot, target, own=False):
        pair, plane, core = block
        source = self.units[unit][0] if own else self.block(unit, *block)
        return pltpu.make_async_remote_copy(
            src_ref=source,
            dst_ref=self.block(unit, *block),
            send_sem=self.send_sem.at[unit, slot],
            recv_sem=self.recv_sem.at[unit, (pair * self.planes + plane) * 2 + core],
            device_id=(target[0], target[1] * 2 + target[2]),
            device_id_type=pl.DeviceIdType.MESH,
        )

    def arrived(self, unit, pair, plane, core):
        here = (self.pair, self.plane, self.core)
        self.copy(unit, (pair, plane, core), 0, here).wait_recv()

    def partners(self, unit):
        order = self.units[unit][4]
        near, far = self.across[order], self.across[1 - order]
        both = self.across[0] + self.across[1] - self.pair
        return near, far, both

    def slot(self, kind, plane):
        return 2 + kind * self.planes + plane

    def spread(self, unit, pair, plane, own=False):
        near, far, _ = self.partners(unit)
        block = (pair, plane, self.core)
        here = (self.plane, self.core)
        self.copy(unit, block, self.slot(1, plane), (near, *here), own).start()
        self.copy(unit, block, self.slot(2, plane), (far, *here), own).start()
        self.copy(unit, block, self.slot(4, plane), (self.pair, self.plane, 1 - self.core), own).start()

    def launch(self, unit):
        block = (self.pair, self.plane, self.core)
        for up in (0, 1):
            step = 2 * up - 1
            inside = (self.plane + step >= 0) & (self.plane + step < self.planes)
            pl.when(inside)(
                lambda up=up, step=step: self.copy(
                    unit, block, up, (self.pair, self.plane + step, self.core), True
                ).start()
            )
        self.spread(unit, self.pair, self.plane, True)

    def along(self, unit, distance):
        for step in (-1, 1):
            origin = self.plane - step * distance
            ahead = self.plane + step

            def take(origin=origin, ahead=ahead):
                self.arrived(unit, self.pair, origin, self.core)
                pl.when((ahead >= 0) & (ahead < self.planes))(
                    lambda: self.copy(
                        unit,
                        (self.pair, origin, self.core),
                        self.slot(0, origin),
                        (self.pair, ahead, self.core),
                    ).start()
                )
                self.spread(unit, self.pair, origin)

            pl.when((origin >= 0) & (origin < self.planes))(take)

    def from_near(self, unit):
        near, far, _ = self.partners(unit)
        for plane in range(self.planes):
            self.arrived(unit, near, plane, self.core)
            block = (near, plane, self.core)
            self.copy(unit, block, self.slot(3, plane), (far, self.plane, self.core)).start()
            self.copy(
                unit, block, self.slot(5, plane), (self.pair, self.plane, 1 - self.core)
            ).start()

    def from_far(self, unit):
        _, far, both = self.partners(unit)
        for kind, pair in ((6, far), (7, both)):
            for plane in range(self.planes):
                self.arrived(unit, pair, plane, self.core)
                self.copy(
                    unit,
                    (pair, plane, self.core),
                    self.slot(kind, plane),
                    (self.pair, self.plane, 1 - self.core),
                ).start()

    def from_core(self, unit):
        near, far, both = self.partners(unit)
        for pair in (self.pair, near, far, both):
            for plane in range(self.planes):
                self.arrived(unit, pair, plane, 1 - self.core)

    def drain(self, unit):
        block = (self.pair, self.plane, self.core)
        here = block

        def sent(slot):
            self.copy(unit, block, slot, here, True).wait_send()

        for up in (0, 1):
            step = 2 * up - 1
            ahead = self.plane + step
            pl.when((ahead >= 0) & (ahead < self.planes))(lambda up=up: sent(up))
            for distance in range(1, self.planes):
                origin = self.plane - step * distance
                inside = (origin >= 0) & (origin < self.planes)
                onward = inside & (ahead >= 0) & (ahead < self.planes)
                pl.when(onward)(lambda origin=origin: sent(self.slot(0, origin)))
        for kind in range(1, 8):
            for plane in range(self.planes):
                sent(self.slot(kind, plane))

    @staticmethod
    def slots(planes):
        return 2 + 8 * planes


def gather_kernel(planes, own, small, *refs):
    parts = own.shape[0]
    wholes, small_whole = refs[:parts], refs[parts]
    local_sem, send_sem, recv_sem = refs[parts + 1 :]
    units = []
    for part in range(parts):
        units += [(own.at[part, half], wholes[part], (), (half,), half) for half in (0, 1)]
        if part == 0:
            units.append((small, small_whole, (), (), 0))
    entry_barrier(planes)
    run = Gather(planes, units, send_sem, recv_sem)
    here = (run.pair, run.plane, run.core)
    keeps = [
        pltpu.make_async_copy(source, run.block(unit, *here), local_sem.at[unit])
        for unit, (source, *_) in enumerate(units)
    ]
    for keep in keeps:
        keep.start()
    groups = [[0, 1, 2]] + [[3 + 2 * i, 4 + 2 * i] for i in range(parts - 1)]

    def each(step, at_group):
        if 0 <= at_group < len(groups):
            for unit in groups[at_group]:
                step(unit)

    def along(at_group):
        for distance in range(1, planes):
            each(lambda unit: run.along(unit, distance), at_group)

    each(run.launch, 0)
    for at_group in range(len(groups) + 2):
        along(at_group)
        each(run.launch, at_group + 1)
        each(run.from_near, at_group - 1)
        each(run.from_far, at_group - 2)
    for unit in range(len(units)):
        run.from_core(unit)
    for unit in range(len(units)):
        run.drain(unit)
    for keep in keeps:
        keep.wait()


def gather_blocks(own, small, planes):
    parts, _, half, width = own.shape
    count = 2 * parts + 1
    anywhere = pl.BlockSpec(memory_space=pl.ANY)
    return pl.pallas_call(
        functools.partial(gather_kernel, planes),
        out_shape=[
            *[jax.ShapeDtypeStruct((4, planes, 2, 2, half, width), own.dtype)] * parts,
            jax.ShapeDtypeStruct((4, planes, 2, *small.shape), small.dtype),
        ],
        in_specs=[anywhere] * 2,
        out_specs=[anywhere] * (parts + 1),
        scratch_shapes=[
            pltpu.SemaphoreType.DMA((count,)),
            pltpu.SemaphoreType.DMA((count, Gather.slots(planes))),
            pltpu.SemaphoreType.DMA((count, 8 * planes)),
        ],
        compiler_params=pltpu.CompilerParams(collective_id=0, has_side_effects=True),
        name="gather_blocks",
    )(own, small)


class Scatter:
    def __init__(self, planes, units, send_sem, recv_sem):
        self.planes, self.units = planes, units
        self.send_sem, self.recv_sem = send_sem, recv_sem
        self.pair, self.plane, self.core, self.across = coordinates(planes)

    def partners(self, unit):
        order = self.units[unit][3]
        near, far = self.across[order], self.across[1 - order]
        return near, far, self.across[0] + self.across[1] - self.pair

    def blocks(self, unit, pair, core):
        whole, before, after = self.units[unit][:3]
        return whole.at[(*before, pair, slice(None), core, *after)]

    def copy(self, unit, slot, source, target, device):
        return pltpu.make_async_remote_copy(
            src_ref=source,
            dst_ref=target,
            send_sem=self.send_sem.at[unit, slot],
            recv_sem=self.recv_sem.at[unit, slot],
            device_id=(device[0], device[1] * 2 + device[2]),
            device_id_type=pl.DeviceIdType.MESH,
        )

    def core_copy(self, unit, pair):
        held = self.units[unit][4]
        return self.copy(
            unit,
            pair,
            self.blocks(unit, pair, 1 - self.core),
            held["core"].at[pair],
            (self.pair, self.plane, 1 - self.core),
        )

    def far_copy(self, unit, which, pair):
        held = self.units[unit][4]
        _, far, _ = self.partners(unit)
        return self.copy(
            unit, 4 + which, held["core"].at[pair], held["far"].at[which], (far, self.plane, self.core)
        )

    def near_copy(self, unit):
        held = self.units[unit][4]
        near, _, _ = self.partners(unit)
        return self.copy(
            unit, 6, held["far"].at[1], held["near"], (near, self.plane, self.core)
        )

    def z_copy(self, unit, up, plane, first):
        held = self.units[unit][4]
        source = held["near"].at[plane] if first else held["z"].at[up, plane]
        step = 2 * up - 1
        return self.copy(
            unit,
            7 + up * self.planes + plane,
            source,
            held["z"].at[up, plane],
            (self.pair, self.plane + step, self.core),
        )

    def local_copy(self, unit, pair, local_sem):
        held = self.units[unit][4]
        return pltpu.make_async_copy(
            self.blocks(unit, pair, self.core), held["own"].at[pair], local_sem.at[unit, pair]
        )

    def launch(self, unit, local_sem):
        near, far, both = self.partners(unit)
        for pair in (both, far, near, self.pair):
            self.core_copy(unit, pair).start()
            self.local_copy(unit, pair, local_sem).start()

    def add(self, target, term):
        def body(i):
            total = target[i].astype(F32) + term[i].astype(F32)
            target[i] = total.astype(target.dtype)

        loop(self.planes, body)

    def from_core(self, unit, local_sem):
        held = self.units[unit][4]
        near, far, both = self.partners(unit)
        for which, pair in ((1, both), (0, far), (None, near), (None, self.pair)):
            self.core_copy(unit, pair).wait_recv()
            self.local_copy(unit, pair, local_sem).wait()
            self.add(held["core"].at[pair], held["own"].at[pair])
            if which is not None:
                self.far_copy(unit, which, pair).start()

    def from_far(self, unit):
        held = self.units[unit][4]
        near, far, both = self.partners(unit)
        self.far_copy(unit, 1, both).wait_recv()
        self.add(held["far"].at[1], held["core"].at[near])
        self.near_copy(unit).start()
        self.far_copy(unit, 0, far).wait_recv()
        self.add(held["far"].at[0], held["core"].at[self.pair])

    def z_cases(self, up):
        step = 2 * up - 1
        behind = self.plane - step
        starts = (behind < 0) | (behind >= self.planes)
        for distance in range(self.planes - 1, 0, -1):
            target = self.plane + step * distance
            inside = (target >= 0) & (target < self.planes)
            yield target, inside & starts, inside & jnp.logical_not(starts)

    def from_near(self, unit):
        held = self.units[unit][4]
        self.near_copy(unit).wait_recv()
        self.add(held["near"], held["far"].at[0])
        for up in (0, 1):
            for target, starts, _ in self.z_cases(up):
                pl.when(starts)(
                    lambda up=up, target=target: self.z_copy(unit, up, target, True).start()
                )

    def from_z(self, unit):
        held = self.units[unit][4]
        for cases in zip(self.z_cases(0), self.z_cases(1)):
            for up, (target, _, passes) in enumerate(cases):

                def go(up=up, target=target):
                    self.z_copy(unit, up, target, False).wait_recv()
                    place = held["z"].at[up, target]
                    total = place[...].astype(F32) + held["near"][target].astype(F32)
                    place[...] = total.astype(place.dtype)
                    self.z_copy(unit, up, target, False).start()

                pl.when(passes)(go)

    def finish(self, unit):
        held, place = self.units[unit][4:]
        place[...] = held["near"][self.plane].astype(F32)
        for up in (0, 1):
            behind = self.plane - (2 * up - 1)

            def take(up=up):
                self.z_copy(unit, up, self.plane, False).wait_recv()
                place[...] += held["z"][up, self.plane].astype(F32)

            pl.when((behind >= 0) & (behind < self.planes))(take)

    def drain(self, unit):
        near, far, both = self.partners(unit)
        for pair in (both, far, near, self.pair):
            self.core_copy(unit, pair).wait_send()
        self.far_copy(unit, 1, both).wait_send()
        self.far_copy(unit, 0, far).wait_send()
        self.near_copy(unit).wait_send()
        for up in (0, 1):
            for target, starts, passes in self.z_cases(up):
                pl.when(starts | passes)(
                    lambda up=up, target=target: self.z_copy(unit, up, target, False).wait_send()
                )

    @staticmethod
    def slots(planes):
        return 7 + 2 * planes

    @staticmethod
    def buffers(planes, block, dtype):
        return [
            pltpu.VMEM((4, planes, *block), dtype),
            pltpu.VMEM((4, planes, *block), dtype),
            pltpu.VMEM((2, planes, *block), dtype),
            pltpu.VMEM((planes, *block), dtype),
            pltpu.VMEM((2, planes, *block), dtype),
        ]


def named(refs, index=None):
    names = ("own", "core", "far", "near", "z")
    return {n: ref if index is None else ref.at[index] for n, ref in zip(names, refs)}


def scatter_kernel(planes, count, *refs):
    wholes, (small_whole,) = refs[:count], refs[count : count + 1]
    outs, (small_out,) = refs[count + 1 : 2 * count + 1], refs[2 * count + 1 : 2 * count + 2]
    rest = refs[2 * count + 2 :]
    local_sem, send_sem, recv_sem = rest[-3:]
    held = rest[:-3]
    entry_barrier(planes)
    units = []
    for part in range(count):
        for half in (0, 1):
            at_unit = 5 * len(units)
            units.append(
                (wholes[part], (), (half,), half, named(held[at_unit : at_unit + 5]), outs[part].at[half])
            )
    units.append((small_whole, (), (), 0, named(held[-5:]), small_out))
    run = Scatter(planes, units, send_sem, recv_sem)
    order = list(range(len(units)))
    order = order[:2] + [order[-1]] + order[2:-1]
    stages = (
        (0, lambda unit: run.launch(unit, local_sem)),
        (1, lambda unit: run.from_core(unit, local_sem)),
        (3, run.from_far),
        (5, run.from_near),
        (7, run.from_z),
        (8, run.finish),
    )
    for at_step in range(len(order) + stages[-1][0]):
        for delay, stage in stages:
            if 0 <= at_step - delay < len(order):
                stage(order[at_step - delay])
    for unit in order:
        run.drain(unit)


def scatter_blocks(wholes, small, planes):
    count = len(wholes)
    block = wholes[0].shape[-2:]
    anywhere = pl.BlockSpec(memory_space=pl.ANY)
    vmem = pl.BlockSpec(memory_space=pltpu.VMEM)
    units = 2 * count + 1
    buffers = []
    for _ in range(2 * count):
        buffers += Scatter.buffers(planes, block, wholes[0].dtype)
    buffers += Scatter.buffers(planes, small.shape[-2:], small.dtype)
    return pl.pallas_call(
        functools.partial(scatter_kernel, planes, count),
        out_shape=[jax.ShapeDtypeStruct((2, *block), F32)] * count
        + [jax.ShapeDtypeStruct(small.shape[-2:], F32)],
        in_specs=[anywhere] * (count + 1),
        out_specs=[vmem] * (count + 1),
        scratch_shapes=[
            *buffers,
            pltpu.SemaphoreType.DMA((units, 4)),
            pltpu.SemaphoreType.DMA((units, Scatter.slots(planes))),
            pltpu.SemaphoreType.DMA((units, Scatter.slots(planes))),
        ],
        compiler_params=pltpu.CompilerParams(
            collective_id=1, has_side_effects=True, vmem_limit_bytes=67043328
        ),
        name="scatter_blocks",
    )(*wholes, small)
def pack_small(pieces, norm_part, multiple):
    owners, _, width = pieces[0].shape
    norm_rows = jnp.pad(norm_part, ((0, 0), (0, -norm_part.shape[1] % width)))
    block = jnp.concatenate([*pieces, norm_rows.reshape(owners, -1, width)], axis=1)
    return jnp.pad(block, ((0, 0), (0, -block.shape[1] % multiple), (0, 0)))


def unpack_small(block, part, count):
    pieces = [block[:, i * part : (i + 1) * part] for i in range(3)]
    return pieces, block[:, 3 * part :].reshape(block.shape[0], -1)[:, :count]


def per_device(
    planes, text_in, layout_in, lengths, attn_text, up_text, down_text,
    attn_layout, up_layout, down_layout, norm_params, grad_text, grad_layout,
):
    width, lwidth = text_in.shape[1], layout_in.shape[1]
    owners = lax.axis_size(AXES)
    text_part, part = down_text.shape[0], down_layout.shape[0]
    count = norm_params.shape[0]
    own_text = [attn_text.T, up_text.T, down_text]
    own_small = pack_small(
        [attn_layout.T[None], up_layout.T[None], down_layout[None]], norm_params[None], 16
    )[0]
    if planes:
        half = text_part // 2
        own = jnp.stack(own_text).reshape(3, 2, half, width)
        *wholes, small = gather_blocks(own, own_small, planes)
        attn, up, down = (whole.reshape(owners * text_part, width) for whole in wholes)
        small = small.reshape(owners, *own_small.shape)
    else:
        gather = lambda piece: lax.all_gather(piece, AXES, axis=0, tiled=True)
        attn, up, down = (gather(piece) for piece in own_text)
        small = gather(own_small[None])
    pieces, norms = unpack_small(small, part, count)
    lattn, lup, ldown = (piece.reshape(owners * part, lwidth) for piece in pieces)
    norms = norms.reshape(-1).astype(F32)
    tnorm = norms[: 4 * width].reshape(4, width)
    lnorm = norms[4 * width :].reshape(4, lwidth)
    (
        text_out, layout_out, dx, dy, gattn, gup, gdown, glattn, glup, gldown, gtnorm, glnorm,
    ) = layer(
        text_in, layout_in, lengths, grad_text, grad_layout, tnorm, lnorm,
        attn, up, down, lattn, lup, ldown,
    )
    gnorm = jnp.concatenate([gtnorm.reshape(-1), glnorm.reshape(-1)]).reshape(owners, count)
    gsmall = pack_small(
        [piece.reshape(owners, part, lwidth) for piece in (glattn, glup, gldown)], gnorm, 16
    ).astype(BF16)
    if planes:
        shape = (4, planes, 2, 2, text_part // 2, width)
        gattn, gup, gdown, gsmall = scatter_blocks(
            [grad.reshape(shape) for grad in (gattn, gup, gdown)],
            gsmall.reshape(4, planes, 2, *gsmall.shape[1:]),
            planes,
        )
        gattn, gup, gdown = (grad.reshape(text_part, width) for grad in (gattn, gup, gdown))
    else:
        scatter = lambda piece: lax.psum_scatter(piece, AXES, scatter_dimension=0, tiled=True)
        gattn, gup, gdown, gsmall = (
            scatter(grad).astype(F32) for grad in (gattn, gup, gdown, gsmall)
        )
        gsmall = gsmall[0]
    pieces, gnorm = unpack_small(gsmall[None], part, count)
    glattn, glup, gldown = (piece[0] for piece in pieces)
    return (
        text_out, layout_out, dx, dy, gattn.T, gup.T, gdown, glattn.T, glup.T, gldown, gnorm[0],
    )


def solution(mesh):
    pairs, columns_on_axis = mesh.shape["dp"], mesh.shape["fsdp"]
    planes = columns_on_axis // 2 if pairs == 4 and columns_on_axis % 2 == 0 else 0
    rows, columns = P(AXES, None), P(None, AXES)
    split = P(AXES)
    return jax.shard_map(
        functools.partial(per_device, planes),
        mesh=mesh,
        in_specs=(
            rows, rows, split, columns, columns, rows, columns, columns, rows, split, rows, rows,
        ),
        out_specs=(rows, rows, rows, rows, columns, columns, rows, columns, columns, rows, split),
        check_vma=False,
    )
```

```python
import functools

import jax
import jax.numpy as jnp
from jax import lax
from jax.experimental import pallas as pl
from jax.experimental.pallas import tpu as pltpu
from jax.sharding import PartitionSpec as P

HEADS = 12
EPSILON = 1e-05
NEG_FILL = -1000000000.0
AXES = ("dp", "fsdp")
BF16 = jnp.bfloat16
F32 = jnp.float32
ROW_STEP = 64


def mm(a, b, dim_a, dim_b):
    return lax.dot_general(a, b, (((dim_a,), (dim_b,)), ((), ())), preferred_element_type=F32)


def loop(count, body):
    def step(i, carry):
        body(i)
        return carry

    lax.fori_loop(0, count, step, 0)


def steps(total, size):
    size = min(size, total)
    assert total % size == 0
    return total // size, size


def at(i, size):
    return pl.ds(pl.multiple_of(i * size, size), size)


def project_heads(x, weight, qkv, scale, chunk):
    width = x.shape[1]
    count, size = steps(width, chunk)

    def body(i):
        block = mm(weight[at(i, size), :], x[...], 1, 1).astype(BF16).astype(F32)
        qkv[at(i, size), :] = (block * jnp.where(i < count, scale, 1.0)).astype(BF16)

    loop(3 * count, body)


def head_rows(ref, part, head, dim, width):
    return ref[pl.ds(pl.multiple_of(part * width + head * dim, dim), dim), :]


def joined(text_ref, layout_ref, part, head, dims, widths):
    return jnp.concatenate(
        [
            head_rows(text_ref, part, head, dims[0], widths[0]),
            head_rows(layout_ref, part, head, dims[1], widths[1]),
        ],
        axis=0,
    )


def masked_scores(query, key, length):
    scores = mm(key, query, 0, 0)
    place = lax.broadcasted_iota(jnp.int32, scores.shape, 0)
    return jnp.where(place < length, scores, NEG_FILL)


def attend_head(head, length, qkv_t, qkv_l, ctx_t, ctx_l, lse, dims, widths):
    query = joined(qkv_t, qkv_l, 0, head, dims, widths)
    key = joined(qkv_t, qkv_l, 1, head, dims, widths)
    value = joined(qkv_t, qkv_l, 2, head, dims, widths)
    scores = masked_scores(query, key, length)
    top = jnp.max(scores, axis=0, keepdims=True)
    grown = jnp.exp(scores - top)
    total = jnp.sum(grown, axis=0, keepdims=True)
    lse[head] = top + jnp.log(total)
    context = mm(value, grown.astype(BF16), 1, 0) * (1.0 / total)
    ctx_t[pl.ds(pl.multiple_of(head * dims[0], dims[0]), dims[0]), :] = context[: dims[0]].astype(BF16)
    ctx_l[pl.ds(pl.multiple_of(head * dims[1], dims[1]), dims[1]), :] = context[dims[0] :].astype(BF16)


def attend_head_back(
    head, length, qkv_t, qkv_l, dctx_t, dctx_l, lse, dqkv_t, dqkv_l, dims, widths, scales
):
    query = joined(qkv_t, qkv_l, 0, head, dims, widths)
    key = joined(qkv_t, qkv_l, 1, head, dims, widths)
    value = joined(qkv_t, qkv_l, 2, head, dims, widths)
    dcontext = joined(dctx_t, dctx_l, 0, head, dims, widths)
    scores = masked_scores(query, key, length)
    probs = jnp.exp(scores - lse[head])
    dvalue = mm(dcontext, probs.astype(BF16), 1, 1)
    dprobs = mm(value, dcontext, 0, 0)
    inner = jnp.sum(dprobs * probs, axis=0, keepdims=True)
    dscores = (probs * (dprobs - inner)).astype(BF16)
    dkey = mm(query, dscores, 1, 1)
    dquery = mm(key, dscores, 1, 0)
    for part, grad in ((0, dquery), (1, dkey), (2, dvalue)):
        for ref, dim, width, scale, rows in (
            (dqkv_t, dims[0], widths[0], scales[0], grad[: dims[0]]),
            (dqkv_l, dims[1], widths[1], scales[1], grad[dims[0] :]),
        ):
            rows = rows * scale if part == 0 else rows
            ref[pl.ds(pl.multiple_of(part * width + head * dim, dim), dim), :] = rows.astype(BF16)


def normed(hidden):
    centred = hidden - jnp.mean(hidden, axis=-1, keepdims=True)
    rate = lax.rsqrt(jnp.mean(centred * centred, axis=-1, keepdims=True) + EPSILON)
    return centred * rate, rate


def norm_back(grad, hat, rate, gain):
    scaled = grad * gain
    mean = jnp.mean(scaled, axis=-1, keepdims=True)
    along = jnp.mean(scaled * hat, axis=-1, keepdims=True)
    return rate * (scaled - mean - hat * along)


def column_sum(values):
    return jnp.sum(values, axis=0, keepdims=True)


def stream_first(x, ctx_tr, ctx, weight, norms, acc, hat, rate, low):
    rows, width = x.shape
    ctx[...] = ctx_tr[...].T
    count, size = steps(rows, 256)

    def product(i):
        acc[at(i, size), :] = mm(ctx[at(i, size), :], weight[3 * width : 4 * width, :], 1, 1)

    loop(count, product)

    def norm(i):
        block = at(i, ROW_STEP)
        hat_b, rate_b = normed(x[block, :].astype(F32) + acc[block, :])
        hat[block, :] = hat_b
        rate[block, :] = rate_b
        low[block, :] = (hat_b * norms[0:1, :] + norms[1:2, :]).astype(BF16)

    loop(rows // ROW_STEP, norm)


def stream_up(low, up, act, slope, chunk):
    count, size = steps(up.shape[0], chunk)

    def body(i):
        block = at(i, size)
        inner = mm(up[block, :], low[...], 1, 1)
        cdf = 0.5 + 0.5 * lax.erf(inner * (0.5**0.5))
        density = jnp.exp(inner * inner * -0.5) * (0.5 / jnp.pi) ** 0.5
        act[block, :] = (inner * cdf).astype(BF16)
        slope[block, :] = (cdf + inner * density).astype(BF16)

    loop(count, body)


def stream_down(act, down, acc, chunk):
    count, size = steps(down.shape[0], chunk)
    acc[...] = mm(act[:size, :], down[:size, :], 0, 0)

    def body(i):
        block = at(i + 1, size)
        acc[...] += mm(act[block, :], down[block, :], 0, 0)

    loop(count - 1, body)


def stream_second(g, norms, acc, hat, out, dhid, dlow, gnorm):
    rows, width = g.shape

    def body(i, sums):
        block = at(i, ROW_STEP)
        hidden = hat[block, :] * norms[0:1, :] + norms[1:2, :] + acc[block, :]
        hat_b, rate_b = normed(hidden)
        out[block, :] = (hat_b * norms[2:3, :] + norms[3:4, :]).astype(BF16)
        grad = g[block, :].astype(F32)
        back = norm_back(grad, hat_b, rate_b, norms[2:3, :])
        dhid[block, :] = back
        dlow[block, :] = back.astype(BF16)
        return sums[0] + column_sum(grad * hat_b), sums[1] + column_sum(grad)

    zero = jnp.zeros((1, width), F32)
    sums = lax.fori_loop(0, rows // ROW_STEP, body, (zero, zero))
    gnorm[2:3, :] = sums[0]
    gnorm[3:4, :] = sums[1]


def stream_inner_back(low, dlow, up, down, act, slope, dhid, gup, gdown, chunk, done):
    count, size = steps(up.shape[0], chunk)

    def body(i):
        block = at(i, size)
        dact = mm(down[block, :], dlow[...], 1, 1)
        dinner = (dact * slope[block, :].astype(F32)).astype(BF16)
        dhid[...] += mm(dinner, up[block, :], 0, 0)
        gdown[block, :] = mm(act[block, :], dlow[...], 1, 0).astype(gdown.dtype)
        gup[block, :] = mm(dinner, low[...], 1, 0).astype(gup.dtype)
        done(i, block)

    loop(count, body)
    return count


def stream_first_back(norms, hat, rate, dhid, dlow, ctx, weight, dctx, gattn, gnorm):
    rows, width = hat.shape

    def body(i, sums):
        block = at(i, ROW_STEP)
        grad = dhid[block, :]
        hat_b = hat[block, :]
        back = norm_back(grad, hat_b, rate[block, :], norms[0:1, :])
        dhid[block, :] = back
        dlow[block, :] = back.astype(BF16)
        return sums[0] + column_sum(grad * hat_b), sums[1] + column_sum(grad)

    zero = jnp.zeros((1, width), F32)
    sums = lax.fori_loop(0, rows // ROW_STEP, body, (zero, zero))
    gnorm[0:1, :] = sums[0]
    gnorm[1:2, :] = sums[1]
    dctx[...] = mm(dlow[...], weight[3 * width : 4 * width, :], 1, 0).astype(BF16).T
    gattn[3 * width : 4 * width, :] = mm(dlow[...], ctx[...], 0, 0).astype(gattn.dtype)


def project_back(x, weight, dqkv, dhid, dx, gattn, chunk, done):
    width = x.shape[1]
    count, size = steps(3 * width, chunk)

    def body(i):
        block = at(i, size)
        dhid[...] += mm(dqkv[block, :], weight[block, :], 0, 0)
        gattn[block, :] = mm(dqkv[block, :], x[...], 1, 0).astype(gattn.dtype)
        done(i, block)

    loop(count, body)
    loop(x.shape[0] // ROW_STEP, lambda i: store_low(dx, dhid, at(i, ROW_STEP)))
    return count


def store_low(out, values, block):
    out[block, :] = values[block, :].astype(BF16)


def layer_kernel(dims, scales, chunks, *refs):
    (
        lengths, x, y, gx, gy, tnorm, lnorm, hattn, hup, hdown, lattn, lup, ldown,
        text_out, layout_out, dx, dy, oattn, oup, odown, glattn, glup, gldown, gtnorm, glnorm,
        attn, up, down, qkv_t, qkv_l, dqkv_t, dqkv_l, ctx_tt, ctx_tl, ctx_t, ctx_l, dctx_t, dctx_l,
        act_t, act_l, slope_t, slope_l, acc_t, acc_l, hat_t, hat_l, dhid_t, dhid_l,
        low_t, low_l, dlow_t, dlow_l, rate_t, rate_l, lse, in_sem, out_sem,
    ) = refs
    widths = (x.shape[1], y.shape[1])
    length = lengths[0]
    loads = [
        pltpu.make_async_copy(src, dst, in_sem.at[i])
        for i, (src, dst) in enumerate(((hattn, attn), (hup, up), (hdown, down)))
    ]
    for load in loads:
        load.start()
    project_heads(y, lattn, qkv_l, scales[1], chunks[1])
    loads[0].wait()
    project_heads(x, attn, qkv_t, scales[0], chunks[0])
    loop(
        HEADS,
        lambda h: attend_head(h, length, qkv_t, qkv_l, ctx_tt, ctx_tl, lse, dims, widths),
    )
    loads[1].wait()
    loads[2].wait()
    nothing = lambda i, block: None
    stream_first(y, ctx_tl, ctx_l, lattn, lnorm, acc_l, hat_l, rate_l, low_l)
    stream_up(low_l, lup, act_l, slope_l, chunks[1])
    stream_down(act_l, ldown, acc_l, chunks[1])
    stream_second(gy, lnorm, acc_l, hat_l, layout_out, dhid_l, dlow_l, glnorm)
    stream_inner_back(
        low_l, dlow_l, lup, ldown, act_l, slope_l, dhid_l, glup, gldown, chunks[1], nothing
    )
    stream_first_back(lnorm, hat_l, rate_l, dhid_l, dlow_l, ctx_l, lattn, dctx_l, glattn, glnorm)

    def send(source, target, block):
        pltpu.make_async_copy(source.at[block, :], target.at[block, :], out_sem).start()

    def sent_inner(i, block):
        send(up, oup, block)
        send(down, odown, block)

    stream_first(x, ctx_tt, ctx_t, attn, tnorm, acc_t, hat_t, rate_t, low_t)
    stream_up(low_t, up, act_t, slope_t, chunks[0])
    stream_down(act_t, down, acc_t, chunks[0])
    stream_second(gx, tnorm, acc_t, hat_t, text_out, dhid_t, dlow_t, gtnorm)
    stream_inner_back(
        low_t, dlow_t, up, down, act_t, slope_t, dhid_t, up, down, chunks[0], sent_inner
    )
    stream_first_back(tnorm, hat_t, rate_t, dhid_t, dlow_t, ctx_t, attn, dctx_t, attn, gtnorm)
    loop(
        HEADS,
        lambda h: attend_head_back(
            h, length, qkv_t, qkv_l, dctx_t, dctx_l, lse, dqkv_t, dqkv_l, dims, widths, scales
        ),
    )
    project_back(y, lattn, dqkv_l, dhid_l, dy, glattn, chunks[1], nothing)
    width = widths[0]
    send(attn, oattn, pl.ds(3 * width, width))
    project_back(
        x, attn, dqkv_t, dhid_t, dx, attn, chunks[0], lambda i, block: send(attn, oattn, block)
    )
    for source, target in ((up, oup), (down, odown), (attn, oattn)):
        pltpu.make_async_copy(source, target, out_sem).wait()


def layer(x, y, lengths, gx, gy, tnorm, lnorm, attn, up, down, lattn, lup, ldown):
    rows, width = x.shape
    lwidth = y.shape[1]
    inner, linner = up.shape[0], lup.shape[0]
    dims = (width // HEADS, lwidth // HEADS)
    scales = tuple(float(dim) ** -0.5 for dim in dims)
    vmem = pl.BlockSpec(memory_space=pltpu.VMEM)
    anywhere = pl.BlockSpec(memory_space=pl.ANY)
    smem = pl.BlockSpec(memory_space=pltpu.SMEM)
    like = jax.ShapeDtypeStruct

    def both(shape_of, dtype):
        return [pltpu.VMEM(shape_of(width, inner), dtype), pltpu.VMEM(shape_of(lwidth, linner), dtype)]

    scratch = [
        pltpu.VMEM(attn.shape, BF16),
        pltpu.VMEM(up.shape, BF16),
        pltpu.VMEM(down.shape, BF16),
        *both(lambda w, f: (3 * w, rows), BF16),
        *both(lambda w, f: (3 * w, rows), BF16),
        *both(lambda w, f: (w, rows), BF16),
        *both(lambda w, f: (rows, w), BF16),
        *both(lambda w, f: (w, rows), BF16),
        *both(lambda w, f: (f, rows), BF16),
        *both(lambda w, f: (f, rows), BF16),
        *both(lambda w, f: (rows, w), F32),
        *both(lambda w, f: (rows, w), F32),
        *both(lambda w, f: (rows, w), F32),
        *both(lambda w, f: (rows, w), BF16),
        *both(lambda w, f: (rows, w), BF16),
        *both(lambda w, f: (rows, 1), F32),
        pltpu.VMEM((HEADS, 1, rows), F32),
        pltpu.SemaphoreType.DMA((3,)),
        pltpu.SemaphoreType.DMA,
    ]
    return pl.pallas_call(
        functools.partial(layer_kernel, dims, scales, (384, 192)),
        out_shape=[
            like(x.shape, BF16),
            like(y.shape, BF16),
            like(x.shape, BF16),
            like(y.shape, BF16),
            like(attn.shape, BF16),
            like(up.shape, BF16),
            like(down.shape, BF16),
            like(lattn.shape, F32),
            like(lup.shape, F32),
            like(ldown.shape, F32),
            like(tnorm.shape, F32),
            like(lnorm.shape, F32),
        ],
        in_specs=[smem] + [vmem] * 6 + [anywhere] * 3 + [vmem] * 3,
        out_specs=[vmem] * 4 + [anywhere] * 3 + [vmem] * 5,
        scratch_shapes=scratch,
        compiler_params=pltpu.CompilerParams(vmem_limit_bytes=67043328),
        name="layer",
    )(lengths, x, y, gx, gy, tnorm, lnorm, attn, up, down, lattn, lup, ldown)


def coordinates(planes):
    pair, column = lax.axis_index("dp"), lax.axis_index("fsdp")
    x, y = lax.rem(pair, 2), pair // 2
    plane, core = column // 2, lax.rem(column, 2)
    across = (pair + 1 - 2 * x, pair + 2 - 4 * y)
    return pair, plane, core, across


def entry_barrier(planes):
    pair, plane, core, across = coordinates(planes)
    barrier = pltpu.get_barrier_semaphore()

    def greet(target_pair, target_plane, target_core):
        pl.semaphore_signal(
            barrier,
            inc=1,
            device_id=(target_pair, target_plane * 2 + target_core),
            device_id_type=pl.DeviceIdType.MESH,
        )

    greet(across[0], plane, core)
    greet(across[1], plane, core)
    greet(pair, plane, 1 - core)
    pl.when(plane > 0)(lambda: greet(pair, plane - 1, core))
    pl.when(plane < planes - 1)(lambda: greet(pair, plane + 1, core))
    edges = jnp.where(plane > 0, 1, 0) + jnp.where(plane < planes - 1, 1, 0)
    pl.semaphore_wait(barrier, 3 + edges)


class Route:
    def __init__(self, planes, units, send_sem, recv_sem):
        self.planes, self.units = planes, units
        self.send_sem, self.recv_sem = send_sem, recv_sem
        self.pair, self.plane, self.core, self.across = coordinates(planes)

    def partners(self, unit):
        order = self.units[unit]["order"]
        near, far = self.across[order], self.across[1 - order]
        return near, far, self.across[0] + self.across[1] - self.pair

    def inside(self, plane):
        return (plane >= 0) & (plane < self.planes)

    def remote(self, source, target, unit, send_slot, recv_slot, device):
        return pltpu.make_async_remote_copy(
            src_ref=source,
            dst_ref=target,
            send_sem=self.send_sem.at[unit, send_slot],
            recv_sem=self.recv_sem.at[unit, recv_slot],
            device_id=(device[0], device[1] * 2 + device[2]),
            device_id_type=pl.DeviceIdType.MESH,
        )


class Gather(Route):
    def copy(self, unit, block, slot, target, own=False):
        pair, plane, core = block
        place = self.units[unit]["place"](*block)
        source = self.units[unit]["own"] if own else place
        arrival = (pair * self.planes + plane) * 2 + core
        return self.remote(source, place, unit, slot, arrival, target)

    def arrived(self, unit, pair, plane, core):
        here = (self.pair, self.plane, self.core)
        self.copy(unit, (pair, plane, core), 0, here).wait_recv()

    def slot(self, kind, plane):
        return 2 + kind * self.planes + plane

    @staticmethod
    def slots(planes):
        return 2 + 8 * planes

    def spread(self, unit, plane, own=False):
        near, far, _ = self.partners(unit)
        block = (self.pair, plane, self.core)
        for kind, pair, core in ((1, near, self.core), (2, far, self.core), (4, self.pair, 1 - self.core)):
            self.copy(unit, block, self.slot(kind, plane), (pair, self.plane, core), own).start()

    def launch(self, unit):
        block = (self.pair, self.plane, self.core)
        for up in (0, 1):
            ahead = self.plane + 2 * up - 1
            pl.when(self.inside(ahead))(
                lambda up=up, ahead=ahead: self.copy(
                    unit, block, up, (self.pair, ahead, self.core), True
                ).start()
            )
        self.spread(unit, self.plane, True)

    def along(self, unit, distance):
        for step in (-1, 1):
            origin, ahead = self.plane - step * distance, self.plane + step

            def take(origin=origin, ahead=ahead):
                self.arrived(unit, self.pair, origin, self.core)
                block = (self.pair, origin, self.core)
                target = (self.pair, ahead, self.core)
                pl.when(self.inside(ahead))(
                    lambda: self.copy(unit, block, self.slot(0, origin), target).start()
                )
                self.spread(unit, origin)

            pl.when(self.inside(origin))(take)

    def from_near(self, unit):
        near, far, _ = self.partners(unit)
        for plane in range(self.planes):
            self.arrived(unit, near, plane, self.core)
            block = (near, plane, self.core)
            for kind, pair, core in ((3, far, self.core), (5, self.pair, 1 - self.core)):
                self.copy(unit, block, self.slot(kind, plane), (pair, self.plane, core)).start()

    def from_far(self, unit):
        _, far, both = self.partners(unit)
        for kind, pair in ((6, far), (7, both)):
            for plane in range(self.planes):
                self.arrived(unit, pair, plane, self.core)
                block = (pair, plane, self.core)
                target = (self.pair, self.plane, 1 - self.core)
                self.copy(unit, block, self.slot(kind, plane), target).start()

    def from_core(self, unit):
        near, far, both = self.partners(unit)
        for pair in (self.pair, near, far, both):
            for plane in range(self.planes):
                self.arrived(unit, pair, plane, 1 - self.core)

    def drain(self, unit):
        here = (self.pair, self.plane, self.core)

        def sent(slot):
            self.copy(unit, here, slot, here, True).wait_send()

        for up in (0, 1):
            step = 2 * up - 1
            ahead = self.inside(self.plane + step)
            pl.when(ahead)(lambda up=up: sent(up))
            for distance in range(1, self.planes):
                origin = self.plane - step * distance
                pl.when(ahead & self.inside(origin))(
                    lambda origin=origin: sent(self.slot(0, origin))
                )
        for kind in range(1, 8):
            for plane in range(self.planes):
                sent(self.slot(kind, plane))


class Scatter(Route):
    @staticmethod
    def slots(planes):
        return 6 * planes + 3

    @staticmethod
    def buffers(planes, block, dtype):
        return [
            pltpu.VMEM((4, planes, *block), dtype),
            pltpu.VMEM((2, planes, *block), dtype),
            pltpu.VMEM((planes, *block), dtype),
            pltpu.VMEM((2, planes, *block), dtype),
        ]

    def copy(self, unit, slot, source, target, device):
        return self.remote(source, target, unit, slot, slot, device)

    def core_copy(self, unit, pair, plane):
        source = self.units[unit]["place"](pair, plane, 1 - self.core)
        target = self.units[unit]["core"].at[pair, plane]
        other = (self.pair, self.plane, 1 - self.core)
        return self.copy(unit, pair * self.planes + plane, source, target, other)

    def far_copy(self, unit, which, pair):
        held = self.units[unit]
        _, far, _ = self.partners(unit)
        target = (far, self.plane, self.core)
        slot = 4 * self.planes + which
        return self.copy(unit, slot, held["core"].at[pair], held["far"].at[which], target)

    def near_copy(self, unit):
        held = self.units[unit]
        near, _, _ = self.partners(unit)
        target = (near, self.plane, self.core)
        return self.copy(unit, 4 * self.planes + 2, held["far"].at[1], held["near"], target)

    def z_copy(self, unit, up, plane, first):
        held = self.units[unit]
        source = held["near"].at[plane] if first else held["z"].at[up, plane]
        target = (self.pair, self.plane + 2 * up - 1, self.core)
        slot = 4 * self.planes + 3 + up * self.planes + plane
        return self.copy(unit, slot, source, held["z"].at[up, plane], target)

    def launch(self, unit, first, count):
        for i in range(count):
            place = first + i
            self.core_copy(unit, place // self.planes, lax.rem(place, self.planes)).start()

    def add(self, target, term_of):
        def body(i):
            total = target[i].astype(F32) + term_of(i).astype(F32)
            target[i] = total.astype(target.dtype)

        loop(self.planes, body)

    def from_core(self, unit):
        held = self.units[unit]
        near, far, both = self.partners(unit)
        for which, pair in ((1, both), (0, far), (None, near), (None, self.pair)):
            for plane in range(self.planes):
                self.core_copy(unit, pair, plane).wait_recv()
            self.add(
                held["core"].at[pair], lambda i, pair=pair: held["place"](pair, i, self.core)[...]
            )
            if which is not None:
                self.far_copy(unit, which, pair).start()

    def from_far(self, unit):
        held = self.units[unit]
        near, far, both = self.partners(unit)
        self.far_copy(unit, 1, both).wait_recv()
        self.add(held["far"].at[1], lambda i: held["core"][near, i])
        self.near_copy(unit).start()
        self.far_copy(unit, 0, far).wait_recv()
        self.add(held["far"].at[0], lambda i: held["core"][self.pair, i])

    def z_cases(self, up):
        step = 2 * up - 1
        starts = jnp.logical_not(self.inside(self.plane - step))
        for distance in range(self.planes - 1, 0, -1):
            target = self.plane + step * distance
            inside = self.inside(target)
            yield target, inside & starts, inside & jnp.logical_not(starts)

    def from_near(self, unit):
        held = self.units[unit]
        self.near_copy(unit).wait_recv()
        self.add(held["near"], lambda i: held["far"][0, i])
        for up in (0, 1):
            for target, starts, _ in self.z_cases(up):
                pl.when(starts)(
                    lambda up=up, target=target: self.z_copy(unit, up, target, True).start()
                )

    def from_z(self, unit):
        held = self.units[unit]
        for cases in zip(self.z_cases(0), self.z_cases(1)):
            for up, (target, _, passes) in enumerate(cases):

                def go(up=up, target=target):
                    self.z_copy(unit, up, target, False).wait_recv()
                    place = held["z"].at[up, target]
                    total = place[...].astype(F32) + held["near"][target].astype(F32)
                    place[...] = total.astype(place.dtype)
                    self.z_copy(unit, up, target, False).start()

                pl.when(passes)(go)

    def finish(self, unit):
        held = self.units[unit]
        result = held["result"]
        result[...] = held["near"][self.plane].astype(F32)
        for up in (0, 1):

            def take(up=up):
                self.z_copy(unit, up, self.plane, False).wait_recv()
                result[...] += held["z"][up, self.plane].astype(F32)

            pl.when(self.inside(self.plane - 2 * up + 1))(take)

    def drain(self, unit):
        near, far, both = self.partners(unit)
        for pair in range(4):
            for plane in range(self.planes):
                self.core_copy(unit, pair, plane).wait_send()
        self.far_copy(unit, 1, both).wait_send()
        self.far_copy(unit, 0, far).wait_send()
        self.near_copy(unit).wait_send()
        for up in (0, 1):
            for target, starts, passes in self.z_cases(up):
                pl.when(starts | passes)(
                    lambda up=up, target=target: self.z_copy(unit, up, target, False).wait_send()
                )


def norm_rows(widths):
    return [-(-width // 128) for width in widths]


def unpack_gathered(small, planes, part, lane_rows, lweights, wide, tnorm, lnorm, norm_sum):
    owners = 4 * planes * 2
    norm_sum[...] = jnp.zeros_like(norm_sum)

    def body(owner):
        block = small[owner // (2 * planes), lax.rem(owner // 2, planes), lax.rem(owner, 2)]
        block = block.astype(F32)
        for i in range(3):
            rows = pl.ds(pl.multiple_of(owner * part, part), part)
            wide[i, rows, :] = block[i * part : (i + 1) * part]
        norm_sum[...] += block[3 * part : 3 * part + norm_sum.shape[0]]

    loop(owners, body)
    for i, weight in enumerate(lweights):
        weight[...] = wide[i].astype(BF16)
    row = 0
    for norm, rows in zip((tnorm, lnorm), lane_rows):
        for i in range(4):
            for j in range(rows):
                lanes = min(128, norm.shape[1] - 128 * j)
                norm[i : i + 1, 128 * j : 128 * j + lanes] = norm_sum[row : row + 1, :lanes]
                row += 1


def pack_grads(small, planes, part, lane_rows, wide, gtnorm, glnorm, norm_sum):
    norm_sum[...] = jnp.zeros_like(norm_sum)
    row = 0
    for norm, rows in zip((gtnorm, glnorm), lane_rows):
        for i in range(4):
            for j in range(rows):
                lanes = min(128, norm.shape[1] - 128 * j)
                norm_sum[row : row + 1, :lanes] = norm[i : i + 1, 128 * j : 128 * j + lanes]
                row += 1
    tail = small.shape[-2] - 3 * part - norm_sum.shape[0]

    def body(owner):
        rows = pl.ds(pl.multiple_of(owner * part, part), part)
        pieces = [wide[i, rows, :] for i in range(3)] + [norm_sum[...]]
        if tail:
            pieces.append(jnp.zeros((tail, small.shape[-1]), F32))
        block = jnp.concatenate(pieces, axis=0).astype(BF16)
        small[owner // (2 * planes), lax.rem(owner // 2, planes), lax.rem(owner, 2)] = block

    loop(4 * planes * 2, body)


def spaced(tasks, first, last):
    by_index = {}
    for i, task in enumerate(tasks):
        place = first + (last - first) * i // max(len(tasks) - 1, 1)
        by_index.setdefault(place, []).append(task)
    return by_index


def heads_beside(body, by_index):
    def step(head):
        for place, tasks in sorted(by_index.items()):

            def run(tasks=tasks):
                for task in tasks:
                    task()

            pl.when(head == place)(run)
        body(head)

    loop(HEADS, step)


def whole_kernel(planes, dims, scales, chunks, part, lpart, *refs):
    (
        lengths, x, y, gx, gy, own, own_small,
        text_out, layout_out, dx, dy, gown_attn, gown_up, gown_down, gown_small,
        attn, up, down, small, lattn, lup, ldown, wide, norm_sum,
        tnorm, lnorm, gtnorm, glnorm,
        qkv_t, qkv_l, ctx_tt, ctx_tl, ctx_t, ctx_l, act_t, act_l, slope_t, slope_l,
        dhid_t, dhid_l, hat_t, hat_l, low_t, low_l, dlow_t, dlow_l, rate_t, rate_l, lse,
        *held,
    ) = refs
    local_sem, gsend, grecv, ssend, srecv = held[-5:]
    widths = (x.shape[1], y.shape[1])
    lane_rows = norm_rows(widths)
    length = lengths[0]
    half_rows = part // 2

    def text_place(whole, half):
        def place(pair, plane, core):
            owner = (pair * planes + plane) * 2 + core
            first = pl.multiple_of(owner * part + half * half_rows, half_rows)
            return whole.at[pl.ds(first, half_rows), :]

        return place

    def small_place(whole):
        return lambda pair, plane, core: whole.at[pair, plane, core]

    gunits, sunits = [], []
    for i, (whole, result) in enumerate(((attn, gown_attn), (up, gown_up), (down, gown_down))):
        for half in (0, 1):
            place = text_place(whole, half)
            gunits.append({"own": own.at[i, half], "place": place, "order": half})
            at_held = 4 * len(sunits)
            sunits.append({"place": place, "order": half, "result": result.at[half]})
            sunits[-1].update(zip(("core", "far", "near", "z"), held[at_held : at_held + 4]))
    gunits.append({"own": own_small, "place": small_place(small), "order": 0})
    sunits.append({"place": small_place(small), "order": 1, "result": gown_small})
    sunits[-1].update(zip(("core", "far", "near", "z"), held[24:28]))
    ATTN, UP, DOWN, SMALL = (0, 1), (2, 3), (4, 5), 6

    entry_barrier(planes)
    gather = Gather(planes, gunits, gsend, grecv)
    scatter = Scatter(planes, sunits, ssend, srecv)
    here = (gather.pair, gather.plane, gather.core)
    keeps = [
        pltpu.make_async_copy(unit["own"], unit["place"](*here), local_sem.at[i])
        for i, unit in enumerate(gunits)
    ]
    for keep in keeps:
        keep.start()

    def task(step, *args):
        return lambda: step(*args)

    def every(step, units, *args):
        for unit in units:
            step(unit, *args)

    first = (*ATTN, SMALL)
    every(gather.launch, first)
    for distance in range(1, planes):
        every(gather.along, first, distance)
    every(gather.launch, UP)
    every(gather.from_near, first)
    for distance in range(1, planes):
        every(gather.along, UP, distance)
    every(gather.from_far, first)
    every(gather.from_core, first)
    for unit in first:
        keeps[unit].wait()

    unpack_gathered(
        small, planes, lpart, lane_rows, (lattn, lup, ldown), wide, tnorm, lnorm, norm_sum
    )
    project_heads(y, lattn, qkv_l, scales[1], chunks[1])
    project_heads(x, attn, qkv_t, scales[0], chunks[0])
    early = [task(every, gather.launch, DOWN), *(task(gather.from_near, unit) for unit in UP)]
    early += [task(every, gather.along, DOWN, distance) for distance in range(1, planes)]
    late = spaced(early, 0, 5)
    late[HEADS - 2] = [task(gather.from_far, UP[0])]
    late[HEADS - 1] = [task(gather.from_far, UP[1])]
    heads_beside(
        lambda h: attend_head(h, length, qkv_t, qkv_l, ctx_tt, ctx_tl, lse, dims, widths), late
    )
    every(gather.from_near, DOWN)
    nothing = lambda i, block: None
    stream_first(y, ctx_tl, ctx_l, lattn, lnorm, dhid_l, hat_l, rate_l, low_l)
    stream_up(low_l, lup, act_l, slope_l, chunks[1])
    stream_down(act_l, ldown, dhid_l, chunks[1])
    stream_second(gy, lnorm, dhid_l, hat_l, layout_out, dhid_l, dlow_l, glnorm)
    every(gather.from_far, DOWN)
    stream_inner_back(
        low_l, dlow_l, lup, ldown, act_l, slope_l, dhid_l, wide.at[1], wide.at[2], chunks[1], nothing
    )
    stream_first_back(
        lnorm, hat_l, rate_l, dhid_l, dlow_l, ctx_l, lattn, ctx_tl, wide.at[0], glnorm
    )
    stream_first(x, ctx_tt, ctx_t, attn, tnorm, dhid_t, hat_t, rate_t, low_t)
    every(gather.from_core, UP)
    for unit in UP:
        keeps[unit].wait()
    stream_up(low_t, up, act_t, slope_t, chunks[0])
    every(gather.from_core, DOWN)
    for unit in DOWN:
        keeps[unit].wait()
    stream_down(act_t, down, dhid_t, chunks[0])
    stream_second(gx, tnorm, dhid_t, hat_t, text_out, dhid_t, dlow_t, gtnorm)
    every(gather.drain, range(len(gunits)))

    by_chunk = chunks[0] // (2 * part)

    def ready(units):
        return lambda i, block: every(scatter.launch, units, i * by_chunk, by_chunk)

    stream_inner_back(
        low_t, dlow_t, up, down, act_t, slope_t, dhid_t, up, down, chunks[0], ready((*UP, *DOWN))
    )
    stream_first_back(tnorm, hat_t, rate_t, dhid_t, dlow_t, ctx_t, attn, ctx_tt, attn, gtnorm)
    every(scatter.launch, ATTN, 3 * planes, planes)
    every(scatter.from_core, (*UP, *DOWN))
    heads_beside(
        lambda h: attend_head_back(
            h, length, qkv_t, qkv_l, ctx_tt, ctx_tl, lse, qkv_t, qkv_l, dims, widths, scales
        ),
        {HEADS - 3: [task(scatter.from_far, UP[0])], HEADS - 2: [task(scatter.from_far, UP[1])]},
    )
    project_back(y, lattn, qkv_l, dhid_l, dy, wide.at[0], chunks[1], nothing)
    pack_grads(small, planes, lpart, lane_rows, wide, gtnorm, glnorm, norm_sum)
    scatter.launch(SMALL, 0, 4 * planes)
    project_back(x, attn, qkv_t, dhid_t, dx, attn, chunks[0], ready(ATTN))
    every(scatter.from_far, DOWN)
    every(scatter.from_core, first)
    every(scatter.from_near, UP)
    every(scatter.from_near, DOWN)
    every(scatter.from_z, UP)
    every(scatter.from_z, DOWN)
    every(scatter.finish, (*UP, *DOWN))
    every(scatter.from_far, first)
    every(scatter.from_near, first)
    every(scatter.from_z, first)
    every(scatter.finish, first)
    every(scatter.drain, range(len(sunits)))


def whole_layer(planes, x, y, lengths, gx, gy, own, own_small, lpart, linner):
    rows, width = x.shape
    lwidth = y.shape[1]
    owners = 4 * planes * 2
    part = 2 * own.shape[2]
    inner = owners * part
    dims = (width // HEADS, lwidth // HEADS)
    scales = tuple(float(dim) ** -0.5 for dim in dims)
    vmem = pl.BlockSpec(memory_space=pltpu.VMEM)
    anywhere = pl.BlockSpec(memory_space=pl.ANY)
    smem = pl.BlockSpec(memory_space=pltpu.SMEM)
    like = jax.ShapeDtypeStruct
    norm_count = 4 * sum(norm_rows((width, lwidth)))
    small = (4, planes, 2, *own_small.shape)

    def both(shape_of, dtype):
        return [pltpu.VMEM(shape_of(width, inner), dtype), pltpu.VMEM(shape_of(lwidth, linner), dtype)]

    held = []
    for _ in range(6):
        held += Scatter.buffers(planes, own.shape[2:], BF16)
    held += Scatter.buffers(planes, own_small.shape, BF16)
    scratch = [
        pltpu.VMEM((inner, width), BF16),
        pltpu.VMEM((inner, width), BF16),
        pltpu.VMEM((inner, width), BF16),
        pltpu.VMEM(small, BF16),
        pltpu.VMEM((linner, lwidth), BF16),
        pltpu.VMEM((linner, lwidth), BF16),
        pltpu.VMEM((linner, lwidth), BF16),
        pltpu.VMEM((3, linner, lwidth), F32),
        pltpu.VMEM((norm_count, lwidth), F32),
        *both(lambda w, f: (4, w), F32),
        *both(lambda w, f: (4, w), F32),
        *both(lambda w, f: (3 * w, rows), BF16),
        *both(lambda w, f: (w, rows), BF16),
        *both(lambda w, f: (rows, w), BF16),
        *both(lambda w, f: (f, rows), BF16),
        *both(lambda w, f: (f, rows), BF16),
        *both(lambda w, f: (rows, w), F32),
        *both(lambda w, f: (rows, w), F32),
        *both(lambda w, f: (rows, w), BF16),
        *both(lambda w, f: (rows, w), BF16),
        *both(lambda w, f: (rows, 1), F32),
        pltpu.VMEM((HEADS, 1, rows), F32),
        *held,
        pltpu.SemaphoreType.DMA((7,)),
        pltpu.SemaphoreType.DMA((7, Gather.slots(planes))),
        pltpu.SemaphoreType.DMA((7, owners)),
        pltpu.SemaphoreType.DMA((7, Scatter.slots(planes))),
        pltpu.SemaphoreType.DMA((7, Scatter.slots(planes))),
    ]
    return pl.pallas_call(
        functools.partial(whole_kernel, planes, dims, scales, (384, 192), part, lpart),
        out_shape=[
            like(x.shape, BF16),
            like(y.shape, BF16),
            like(x.shape, BF16),
            like(y.shape, BF16),
            *[like(own.shape[1:], F32)] * 3,
            like(own_small.shape, F32),
        ],
        in_specs=[smem] + [vmem] * 4 + [anywhere] * 2,
        out_specs=[vmem] * 8,
        scratch_shapes=scratch,
        compiler_params=pltpu.CompilerParams(
            collective_id=0, has_side_effects=True, vmem_limit_bytes=67043328
        ),
        name="whole_layer",
    )(lengths, x, y, gx, gy, own, own_small)


def pack_small(pieces, norm_part, multiple):
    owners, _, width = pieces[0].shape
    norm_part = jnp.pad(norm_part, ((0, 0), (0, -norm_part.shape[1] % width)))
    block = jnp.concatenate([*pieces, norm_part.reshape(owners, -1, width)], axis=1)
    return jnp.pad(block, ((0, 0), (0, -block.shape[1] % multiple), (0, 0)))


def unpack_small(block, part, count):
    pieces = [block[:, i * part : (i + 1) * part] for i in range(3)]
    return pieces, block[:, 3 * part :].reshape(block.shape[0], -1)[:, :count]


def lanes_of(flat, widths):
    pieces, first = [], 0
    for width in widths:
        piece = flat[first : first + 4 * width].reshape(4, width)
        first += 4 * width
        pieces.append(jnp.pad(piece, ((0, 0), (0, -width % 128))).reshape(-1, 128))
    return jnp.concatenate(pieces, axis=0)


def flat_of(lanes, widths):
    pieces, first = [], 0
    for width, rows in zip(widths, norm_rows(widths)):
        piece = lanes[first : first + 4 * rows].reshape(4, rows * 128)
        first += 4 * rows
        pieces.append(piece[:, :width].reshape(-1))
    return jnp.concatenate(pieces)


def by_kernel(
    planes, text_in, layout_in, lengths, attn_text, up_text, down_text,
    attn_layout, up_layout, down_layout, norm_params, grad_text, grad_layout,
):
    width, lwidth = text_in.shape[1], layout_in.shape[1]
    owners = lax.axis_size(AXES)
    text_part, part = down_text.shape[0], down_layout.shape[0]
    count = norm_params.shape[0]
    own = jnp.stack([attn_text.T, up_text.T, down_text]).reshape(3, 2, text_part // 2, width)
    first = lax.axis_index(AXES) * count
    spread = jnp.pad(norm_params, ((owners - 1) * count, (owners - 1) * count))
    spread = lax.dynamic_slice(spread, ((owners - 1) * count - first,), (owners * count,))
    lanes = lanes_of(spread, (width, lwidth))
    lanes = jnp.pad(lanes, ((0, 0), (0, lwidth - 128)))
    small = jnp.concatenate([attn_layout.T, up_layout.T, down_layout, lanes], axis=0)
    small = jnp.pad(small, ((0, -small.shape[0] % 16), (0, 0)))
    text_out, layout_out, dx, dy, gattn, gup, gdown, gsmall = whole_layer(
        planes, text_in, layout_in, lengths, grad_text, grad_layout, own, small,
        part, owners * part,
    )
    gattn, gup, gdown = (grad.reshape(text_part, width) for grad in (gattn, gup, gdown))
    glattn, glup, gldown = (gsmall[i * part : (i + 1) * part] for i in range(3))
    gnorm = gsmall[3 * part : 3 * part + lanes.shape[0], :128]
    gnorm = lax.dynamic_slice(flat_of(gnorm, (width, lwidth)), (first,), (count,))
    return text_out, layout_out, dx, dy, gattn.T, gup.T, gdown, glattn.T, glup.T, gldown, gnorm


def by_collectives(
    text_in, layout_in, lengths, attn_text, up_text, down_text,
    attn_layout, up_layout, down_layout, norm_params, grad_text, grad_layout,
):
    width, lwidth = text_in.shape[1], layout_in.shape[1]
    owners = lax.axis_size(AXES)
    part, count = down_layout.shape[0], norm_params.shape[0]

    def gather(piece):
        return lax.all_gather(piece, AXES, axis=0, tiled=True)

    def scatter(piece):
        return lax.psum_scatter(piece, AXES, scatter_dimension=0, tiled=True)

    small = pack_small(
        [attn_layout.T[None], up_layout.T[None], down_layout[None]], norm_params[None], 16
    )
    pieces, norms = unpack_small(gather(small), part, count)
    lattn, lup, ldown = (piece.reshape(owners * part, lwidth) for piece in pieces)
    norms = norms.reshape(-1).astype(F32)
    tnorm = norms[: 4 * width].reshape(4, width)
    lnorm = norms[4 * width :].reshape(4, lwidth)
    attn, up, down = gather(attn_text.T), gather(up_text.T), gather(down_text)
    (
        text_out, layout_out, dx, dy, gattn, gup, gdown, glattn, glup, gldown, gtnorm, glnorm,
    ) = layer(
        text_in, layout_in, lengths, grad_text, grad_layout, tnorm, lnorm,
        attn, up, down, lattn, lup, ldown,
    )
    gnorm = jnp.concatenate([gtnorm.reshape(-1), glnorm.reshape(-1)]).reshape(owners, count)
    gsmall = pack_small(
        [piece.reshape(owners, part, lwidth) for piece in (glattn, glup, gldown)], gnorm, 16
    )
    gattn, gup, gdown, gsmall = (
        scatter(grad).astype(F32) for grad in (gattn, gup, gdown, gsmall)
    )
    (glattn, glup, gldown), gnorm = unpack_small(gsmall, part, count)
    return (
        text_out, layout_out, dx, dy, gattn.T, gup.T, gdown,
        glattn[0].T, glup[0].T, gldown[0], gnorm[0],
    )


def solution(mesh):
    pairs, columns_on_axis = mesh.shape["dp"], mesh.shape["fsdp"]
    body = by_collectives
    if pairs == 4 and columns_on_axis % 2 == 0 and columns_on_axis <= 8:
        body = functools.partial(by_kernel, columns_on_axis // 2)
    rows, columns = P(AXES, None), P(None, AXES)
    split = P(AXES)
    return jax.shard_map(
        body,
        mesh=mesh,
        in_specs=(
            rows, rows, split, columns, columns, rows, columns, columns, rows, split, rows, rows,
        ),
        out_specs=(rows, rows, rows, rows, columns, columns, rows, columns, columns, rows, split),
        check_vma=False,
    )
```

```python
import functools

import jax
import jax.numpy as jnp
from jax import lax
from jax.experimental import pallas as pl
from jax.experimental.pallas import tpu as pltpu
from jax.sharding import PartitionSpec as P

HEADS = 12
EPSILON = 1e-05
NEG_FILL = -1000000000.0
AXES = ("dp", "fsdp")
BF16 = jnp.bfloat16
F32 = jnp.float32
ROW_STEP = 64


def mm(a, b, dim_a, dim_b):
    return lax.dot_general(a, b, (((dim_a,), (dim_b,)), ((), ())), preferred_element_type=F32)


def loop(count, body):
    def step(i, carry):
        body(i)
        return carry

    lax.fori_loop(0, count, step, 0)


def steps(total, size):
    size = min(size, total)
    assert total % size == 0
    return total // size, size


def at(i, size):
    return pl.ds(pl.multiple_of(i * size, size), size)


def project_heads(x, weight, qkv, scale, chunk):
    width = x.shape[1]
    count, size = steps(width, chunk)

    def body(i):
        block = mm(weight[at(i, size), :], x[...], 1, 1).astype(BF16).astype(F32)
        qkv[at(i, size), :] = (block * jnp.where(i < count, scale, 1.0)).astype(BF16)

    loop(3 * count, body)


def head_rows(ref, part, head, dim, width):
    return ref[pl.ds(pl.multiple_of(part * width + head * dim, dim), dim), :]


def joined(text_ref, layout_ref, part, head, dims, widths):
    return jnp.concatenate(
        [
            head_rows(text_ref, part, head, dims[0], widths[0]),
            head_rows(layout_ref, part, head, dims[1], widths[1]),
        ],
        axis=0,
    )


def masked_scores(query, key, length):
    scores = mm(key, query, 0, 0)
    place = lax.broadcasted_iota(jnp.int32, scores.shape, 0)
    return jnp.where(place < length, scores, NEG_FILL)


def attend_head(head, length, qkv_t, qkv_l, ctx_t, ctx_l, lse, dims, widths):
    query = joined(qkv_t, qkv_l, 0, head, dims, widths)
    key = joined(qkv_t, qkv_l, 1, head, dims, widths)
    value = joined(qkv_t, qkv_l, 2, head, dims, widths)
    scores = masked_scores(query, key, length)
    top = jnp.max(scores, axis=0, keepdims=True)
    grown = jnp.exp(scores - top)
    total = jnp.sum(grown, axis=0, keepdims=True)
    lse[head] = top + jnp.log(total)
    context = mm(value, grown.astype(BF16), 1, 0) * (1.0 / total)
    ctx_t[pl.ds(pl.multiple_of(head * dims[0], dims[0]), dims[0]), :] = context[: dims[0]].astype(BF16)
    ctx_l[pl.ds(pl.multiple_of(head * dims[1], dims[1]), dims[1]), :] = context[dims[0] :].astype(BF16)


def attend_head_back(
    head, length, qkv_t, qkv_l, dctx_t, dctx_l, lse, dqkv_t, dqkv_l, dims, widths, scales
):
    query = joined(qkv_t, qkv_l, 0, head, dims, widths)
    key = joined(qkv_t, qkv_l, 1, head, dims, widths)
    value = joined(qkv_t, qkv_l, 2, head, dims, widths)
    dcontext = joined(dctx_t, dctx_l, 0, head, dims, widths)
    scores = masked_scores(query, key, length)
    probs = jnp.exp(scores - lse[head])
    dvalue = mm(dcontext, probs.astype(BF16), 1, 1)
    dprobs = mm(value, dcontext, 0, 0)
    inner = jnp.sum(dprobs * probs, axis=0, keepdims=True)
    dscores = (probs * (dprobs - inner)).astype(BF16)
    dkey = mm(query, dscores, 1, 1)
    dquery = mm(key, dscores, 1, 0)
    for part, grad in ((0, dquery), (1, dkey), (2, dvalue)):
        for ref, dim, width, scale, rows in (
            (dqkv_t, dims[0], widths[0], scales[0], grad[: dims[0]]),
            (dqkv_l, dims[1], widths[1], scales[1], grad[dims[0] :]),
        ):
            rows = rows * scale if part == 0 else rows
            ref[pl.ds(pl.multiple_of(part * width + head * dim, dim), dim), :] = rows.astype(BF16)


def normed(hidden):
    centred = hidden - jnp.mean(hidden, axis=-1, keepdims=True)
    rate = lax.rsqrt(jnp.mean(centred * centred, axis=-1, keepdims=True) + EPSILON)
    return centred * rate, rate


def norm_back(grad, hat, rate, gain):
    scaled = grad * gain
    mean = jnp.mean(scaled, axis=-1, keepdims=True)
    along = jnp.mean(scaled * hat, axis=-1, keepdims=True)
    return rate * (scaled - mean - hat * along)


def column_sum(values):
    return jnp.sum(values, axis=0, keepdims=True)


def stream_first(x, ctx_tr, ctx, weight, norms, acc, hat, rate, low):
    rows, width = x.shape
    ctx[...] = ctx_tr[...].T
    count, size = steps(rows, 256)

    def product(i):
        acc[at(i, size), :] = mm(ctx[at(i, size), :], weight[3 * width : 4 * width, :], 1, 1)

    loop(count, product)

    def norm(i):
        block = at(i, ROW_STEP)
        hat_b, rate_b = normed(x[block, :].astype(F32) + acc[block, :])
        hat[block, :] = hat_b
        rate[block, :] = rate_b
        low[block, :] = (hat_b * norms[0:1, :] + norms[1:2, :]).astype(BF16)

    loop(rows // ROW_STEP, norm)


def stream_up(low, up, act, slope, chunk):
    count, size = steps(up.shape[0], chunk)

    def body(i):
        block = at(i, size)
        inner = mm(up[block, :], low[...], 1, 1)
        cdf = 0.5 + 0.5 * lax.erf(inner * (0.5**0.5))
        density = jnp.exp(inner * inner * -0.5) * (0.5 / jnp.pi) ** 0.5
        act[block, :] = (inner * cdf).astype(BF16)
        slope[block, :] = (cdf + inner * density).astype(BF16)

    loop(count, body)


def stream_down(act, down, acc, chunk):
    count, size = steps(down.shape[0], chunk)
    acc[...] = mm(act[:size, :], down[:size, :], 0, 0)

    def body(i):
        block = at(i + 1, size)
        acc[...] += mm(act[block, :], down[block, :], 0, 0)

    loop(count - 1, body)


def stream_second(g, norms, acc, hat, out, dhid, dlow, gnorm):
    rows, width = g.shape

    def body(i, sums):
        block = at(i, ROW_STEP)
        hidden = hat[block, :] * norms[0:1, :] + norms[1:2, :] + acc[block, :]
        hat_b, rate_b = normed(hidden)
        grad = g[block, :].astype(F32)
        out[block, :] = (hat_b * norms[2:3, :] + norms[3:4, :]).astype(BF16)
        back = norm_back(grad, hat_b, rate_b, norms[2:3, :])
        dhid[block, :] = back
        dlow[block, :] = back.astype(BF16)
        return sums[0] + column_sum(grad * hat_b), sums[1] + column_sum(grad)

    zero = jnp.zeros((1, width), F32)
    sums = lax.fori_loop(0, rows // ROW_STEP, body, (zero, zero))
    gnorm[2:3, :] = sums[0]
    gnorm[3:4, :] = sums[1]


def stream_inner_back(
    low, dlow, up, down, act, slope, dhid, gup, gdown, chunk, done, chunk_of=lambda i: i
):
    count, size = steps(up.shape[0], chunk)

    def body(i):
        block = at(chunk_of(i), size)
        dact = mm(down[block, :], dlow[...], 1, 1)
        dinner = (dact * slope[block, :].astype(F32)).astype(BF16)
        dhid[...] += mm(dinner, up[block, :], 0, 0)
        gdown[block, :] = mm(act[block, :], dlow[...], 1, 0).astype(gdown.dtype)
        gup[block, :] = mm(dinner, low[...], 1, 0).astype(gup.dtype)
        done(i, block)

    loop(count, body)
    return count


def stream_first_back(norms, hat, rate, dhid, dlow, ctx, weight, dctx, gattn, gnorm):
    rows, width = hat.shape

    def body(i, sums):
        block = at(i, ROW_STEP)
        grad = dhid[block, :]
        hat_b = hat[block, :]
        back = norm_back(grad, hat_b, rate[block, :], norms[0:1, :])
        dhid[block, :] = back
        dlow[block, :] = back.astype(BF16)
        return sums[0] + column_sum(grad * hat_b), sums[1] + column_sum(grad)

    zero = jnp.zeros((1, width), F32)
    sums = lax.fori_loop(0, rows // ROW_STEP, body, (zero, zero))
    gnorm[0:1, :] = sums[0]
    gnorm[1:2, :] = sums[1]
    dctx[...] = mm(dlow[...], weight[3 * width : 4 * width, :], 1, 0).astype(BF16).T
    gattn[3 * width : 4 * width, :] = mm(dlow[...], ctx[...], 0, 0).astype(gattn.dtype)


def project_back(x, weight, dqkv, dhid, dx, gattn, chunk, done):
    width = x.shape[1]
    count, size = steps(3 * width, chunk)

    def body(i):
        block = at(i, size)
        dhid[...] += mm(dqkv[block, :], weight[block, :], 0, 0)
        gattn[block, :] = mm(dqkv[block, :], x[...], 1, 0).astype(gattn.dtype)
        done(i, block)

    loop(count, body)
    loop(x.shape[0] // ROW_STEP, lambda i: store_low(dx, dhid, at(i, ROW_STEP)))
    return count


def store_low(out, values, block):
    out[block, :] = values[block, :].astype(BF16)


def layer_kernel(dims, scales, chunks, *refs):
    (
        lengths, x, y, gx, gy, tnorm, lnorm, hattn, hup, hdown, lattn, lup, ldown,
        text_out, layout_out, dx, dy, oattn, oup, odown, glattn, glup, gldown, gtnorm, glnorm,
        attn, up, down, qkv_t, qkv_l, dqkv_t, dqkv_l, ctx_tt, ctx_tl, ctx_t, ctx_l, dctx_t, dctx_l,
        act_t, act_l, slope_t, slope_l, acc_t, acc_l, hat_t, hat_l, dhid_t, dhid_l,
        low_t, low_l, dlow_t, dlow_l, rate_t, rate_l, lse, in_sem, out_sem,
    ) = refs
    widths = (x.shape[1], y.shape[1])
    length = lengths[0]
    loads = [
        pltpu.make_async_copy(src, dst, in_sem.at[i])
        for i, (src, dst) in enumerate(((hattn, attn), (hup, up), (hdown, down)))
    ]
    for load in loads:
        load.start()
    project_heads(y, lattn, qkv_l, scales[1], chunks[1])
    loads[0].wait()
    project_heads(x, attn, qkv_t, scales[0], chunks[0])
    loop(
        HEADS,
        lambda h: attend_head(h, length, qkv_t, qkv_l, ctx_tt, ctx_tl, lse, dims, widths),
    )
    loads[1].wait()
    loads[2].wait()
    nothing = lambda i, block: None
    stream_first(y, ctx_tl, ctx_l, lattn, lnorm, acc_l, hat_l, rate_l, low_l)
    stream_up(low_l, lup, act_l, slope_l, chunks[1])
    stream_down(act_l, ldown, acc_l, chunks[1])
    stream_second(gy, lnorm, acc_l, hat_l, layout_out, dhid_l, dlow_l, glnorm)
    stream_inner_back(
        low_l, dlow_l, lup, ldown, act_l, slope_l, dhid_l, glup, gldown, chunks[1], nothing
    )
    stream_first_back(lnorm, hat_l, rate_l, dhid_l, dlow_l, ctx_l, lattn, dctx_l, glattn, glnorm)

    def send(source, target, block):
        pltpu.make_async_copy(source.at[block, :], target.at[block, :], out_sem).start()

    def sent_inner(i, block):
        send(up, oup, block)
        send(down, odown, block)

    stream_first(x, ctx_tt, ctx_t, attn, tnorm, acc_t, hat_t, rate_t, low_t)
    stream_up(low_t, up, act_t, slope_t, chunks[0])
    stream_down(act_t, down, acc_t, chunks[0])
    stream_second(gx, tnorm, acc_t, hat_t, text_out, dhid_t, dlow_t, gtnorm)
    stream_inner_back(
        low_t, dlow_t, up, down, act_t, slope_t, dhid_t, up, down, chunks[0], sent_inner
    )
    stream_first_back(tnorm, hat_t, rate_t, dhid_t, dlow_t, ctx_t, attn, dctx_t, attn, gtnorm)
    loop(
        HEADS,
        lambda h: attend_head_back(
            h, length, qkv_t, qkv_l, dctx_t, dctx_l, lse, dqkv_t, dqkv_l, dims, widths, scales
        ),
    )
    project_back(y, lattn, dqkv_l, dhid_l, dy, glattn, chunks[1], nothing)
    width = widths[0]
    send(attn, oattn, pl.ds(3 * width, width))
    project_back(
        x, attn, dqkv_t, dhid_t, dx, attn, chunks[0], lambda i, block: send(attn, oattn, block)
    )
    for source, target in ((up, oup), (down, odown), (attn, oattn)):
        pltpu.make_async_copy(source, target, out_sem).wait()


def layer(x, y, lengths, gx, gy, tnorm, lnorm, attn, up, down, lattn, lup, ldown):
    rows, width = x.shape
    lwidth = y.shape[1]
    inner, linner = up.shape[0], lup.shape[0]
    dims = (width // HEADS, lwidth // HEADS)
    scales = tuple(float(dim) ** -0.5 for dim in dims)
    vmem = pl.BlockSpec(memory_space=pltpu.VMEM)
    anywhere = pl.BlockSpec(memory_space=pl.ANY)
    smem = pl.BlockSpec(memory_space=pltpu.SMEM)
    like = jax.ShapeDtypeStruct

    def both(shape_of, dtype):
        return [pltpu.VMEM(shape_of(width, inner), dtype), pltpu.VMEM(shape_of(lwidth, linner), dtype)]

    scratch = [
        pltpu.VMEM(attn.shape, BF16),
        pltpu.VMEM(up.shape, BF16),
        pltpu.VMEM(down.shape, BF16),
        *both(lambda w, f: (3 * w, rows), BF16),
        *both(lambda w, f: (3 * w, rows), BF16),
        *both(lambda w, f: (w, rows), BF16),
        *both(lambda w, f: (rows, w), BF16),
        *both(lambda w, f: (w, rows), BF16),
        *both(lambda w, f: (f, rows), BF16),
        *both(lambda w, f: (f, rows), BF16),
        *both(lambda w, f: (rows, w), F32),
        *both(lambda w, f: (rows, w), F32),
        *both(lambda w, f: (rows, w), F32),
        *both(lambda w, f: (rows, w), BF16),
        *both(lambda w, f: (rows, w), BF16),
        *both(lambda w, f: (rows, 1), F32),
        pltpu.VMEM((HEADS, 1, rows), F32),
        pltpu.SemaphoreType.DMA((3,)),
        pltpu.SemaphoreType.DMA,
    ]
    return pl.pallas_call(
        functools.partial(layer_kernel, dims, scales, (384, 192)),
        out_shape=[
            like(x.shape, BF16),
            like(y.shape, BF16),
            like(x.shape, BF16),
            like(y.shape, BF16),
            like(attn.shape, BF16),
            like(up.shape, BF16),
            like(down.shape, BF16),
            like(lattn.shape, F32),
            like(lup.shape, F32),
            like(ldown.shape, F32),
            like(tnorm.shape, F32),
            like(lnorm.shape, F32),
        ],
        in_specs=[smem] + [vmem] * 6 + [anywhere] * 3 + [vmem] * 3,
        out_specs=[vmem] * 4 + [anywhere] * 3 + [vmem] * 5,
        scratch_shapes=scratch,
        compiler_params=pltpu.CompilerParams(vmem_limit_bytes=67043328),
        name="layer",
    )(lengths, x, y, gx, gy, tnorm, lnorm, attn, up, down, lattn, lup, ldown)


SECOND_APART = True

GATHER_PLAN = (
    (0, "launch", 7),
    (0, "launch", 3),
    (0, "along", 3, 1),
    (0, "launch", 5),
    (0, "launch", 2),
    (1, "from_near", 7),
    (1, "along", 2, 1),
    (2, "launch", 4),
    (3, "along", 2, 2),
    (4, "along", 3, 2),
    (4, "from_far", 7),
    (5, "along", 4, 1),
    (7, "along", 7, 1),
    (8, "along", 2, 3),
    (8, "along", 3, 3),
    (10, "from_near", 2),
    (10, "from_near", 3),
    (11, "along", 7, 2),
    (13, "along", 5, 1),
    (13, "along", 7, 3),
    (13, "along", 5, 2),
    (14, "along", 4, 2),
    (15, "from_far", 2),
    (16, "from_far", 3),
    (16, "along", 5, 3),
    (16, "along", 4, 3),
    (19, "from_near", 4),
    (19, "from_near", 5),
    (20, "from_far", 5),
    (20, "from_far", 4),
)
SCATTER_PLAN = (
    (2, "from_core", 2, 0),
    (3, "from_core", 3, 0),
    (4, "from_core", 4, 0),
    (5, "from_core", 2, 1),
    (5, "from_core", 5, 0),
    (7, "from_core", 4, 1),
    (7, "from_core", 3, 1),
    (9, "from_core", 3, 2),
    (9, "from_core", 4, 2),
    (11, "from_core", 5, 1),
    (11, "from_core", 3, 3),
    (11, "from_core", 7, 0),
    (11, "from_core", 7, 1),
    (11, "from_core", 7, 2),
    (12, "from_core", 7, 3),
    (13, "from_core", 5, 2),
    (13, "from_core", 2, 2),
    (14, "from_far", 3),
    (15, "from_core", 5, 3),
    (15, "from_core", 4, 3),
    (17, "from_core", 2, 3),
    (19, "from_far", 4),
    (20, "from_z", 7, 1),
    (21, "from_near", 3),
    (23, "from_far", 2),
    (25, "from_core", 6, 0),
    (25, "from_core", 6, 1),
    (25, "from_core", 6, 2),
    (25, "from_core", 6, 3),
    (25, "from_z", 7, 2),
    (27, "from_near", 4),
    (27, "from_far", 5),
    (29, "from_near", 2),
    (30, "from_z", 3, 1),
    (30, "from_far", 6),
    (30, "finish", 7),
    (31, "from_z", 3, 2),
    (31, "from_near", 5),
    (31, "from_z", 4, 1),
    (31, "from_far", 7),
    (31, "from_near", 6),
    (31, "from_z", 2, 1),
    (32, "from_core", 0, 0),
    (32, "from_core", 1, 0),
    (32, "from_near", 7),
    (32, "from_z", 6, 1),
    (32, "from_core", 0, 1),
    (32, "from_z", 5, 1),
    (32, "from_core", 0, 2),
    (32, "from_z", 6, 2),
    (32, "from_z", 2, 2),
    (32, "from_core", 0, 3),
    (32, "from_core", 1, 1),
    (32, "from_far", 0),
    (32, "from_core", 1, 2),
    (32, "from_z", 4, 2),
    (32, "from_core", 1, 3),
    (32, "from_z", 5, 2),
    (32, "from_near", 0),
    (32, "from_z", 0, 1),
    (32, "finish", 4),
    (32, "finish", 6),
    (32, "from_far", 1),
    (32, "from_z", 0, 2),
    (32, "from_near", 1),
    (32, "from_z", 1, 1),
    (32, "finish", 3),
    (32, "finish", 2),
    (32, "finish", 5),
    (32, "from_z", 1, 2),
    (32, "finish", 0),
    (32, "finish", 1),
)


def coordinates(planes):
    pair, column = lax.axis_index("dp"), lax.axis_index("fsdp")
    x, y = lax.rem(pair, 2), pair // 2
    plane, core = column // 2, lax.rem(column, 2)
    across = (pair + 1 - 2 * x, pair + 2 - 4 * y)
    return pair, plane, core, across


def entry_barrier(planes):
    pair, plane, core, across = coordinates(planes)
    barrier = pltpu.get_barrier_semaphore()

    def greet(target_pair, target_plane, target_core):
        pl.semaphore_signal(
            barrier,
            inc=1,
            device_id=(target_pair, target_plane * 2 + target_core),
            device_id_type=pl.DeviceIdType.MESH,
        )

    greet(across[0], plane, core)
    greet(across[1], plane, core)
    greet(pair, plane, 1 - core)
    pl.when(plane > 0)(lambda: greet(pair, plane - 1, core))
    pl.when(plane < planes - 1)(lambda: greet(pair, plane + 1, core))
    edges = jnp.where(plane > 0, 1, 0) + jnp.where(plane < planes - 1, 1, 0)
    pl.semaphore_wait(barrier, 3 + edges)


class Route:
    def __init__(self, planes, units, send_sem, recv_sem):
        self.planes, self.units = planes, units
        self.send_sem, self.recv_sem = send_sem, recv_sem
        self.pair, self.plane, self.core, self.across = coordinates(planes)

    def partners(self, unit):
        order = self.units[unit]["order"]
        near, far = self.across[order], self.across[1 - order]
        return near, far, self.across[0] + self.across[1] - self.pair

    def turn(self, index):
        near, far = self.across
        order = (near + far - self.pair, far, near, self.pair)
        if isinstance(index, int):
            return order[index]
        later = jnp.where(index == 2, order[2], order[3])
        return jnp.where(index == 0, order[0], jnp.where(index == 1, order[1], later))

    def inside(self, plane):
        return (plane >= 0) & (plane < self.planes)

    def remote(self, source, target, unit, send_slot, recv_slot, device):
        return pltpu.make_async_remote_copy(
            src_ref=source,
            dst_ref=target,
            send_sem=self.send_sem.at[unit, send_slot],
            recv_sem=self.recv_sem.at[unit, recv_slot],
            device_id=(device[0], device[1] * 2 + device[2]),
            device_id_type=pl.DeviceIdType.MESH,
        )


class Gather(Route):
    @staticmethod
    def send_slots(planes):
        return 3 + planes

    @staticmethod
    def arrival_slots(planes):
        return 5 * planes + 1

    def copy(self, unit, block, slot, arrival, target, own=False):
        place = self.units[unit]["place"](*block)
        source = self.units[unit]["own"] if own else place
        return self.remote(source, place, unit, slot, arrival, target)

    def arrival(self, block):
        return block[0] * self.planes + block[1]

    def share(self, unit, block, pair, own=False):
        target = (pair, self.plane, self.core)
        self.copy(unit, block, 2 + self.planes, self.arrival(block), target, own).start()

    def to_core(self, unit, block, own=False):
        target = (self.pair, self.plane, 1 - self.core)
        self.copy(unit, block, 2 + self.planes, 5 * self.planes, target, own).start()

    def arrived(self, unit, pair, plane):
        here = (self.pair, self.plane, self.core)
        block = (pair, plane, self.core)
        self.copy(unit, block, 0, self.arrival(block), here).wait_recv()

    def wait_blocks(self, unit, count, semaphore):
        sized = self.units[unit]["sized"](count)
        pltpu.make_async_copy(sized, sized, semaphore).wait()

    def ahead(self, step):
        return (self.pair, self.plane + step, self.core)

    def spread(self, unit, plane, own=False):
        near, far, _ = self.partners(unit)
        block = (self.pair, plane, self.core)
        self.share(unit, block, near, own)
        self.share(unit, block, far, own)
        self.to_core(unit, block, own)

    def launch(self, unit):
        block = (self.pair, self.plane, self.core)
        if not self.units[unit]["z_last"]:
            for up in (0, 1):
                step = 2 * up - 1
                send = lambda up=up, step=step: self.copy(
                    unit, block, up, self.arrival(block), self.ahead(step), True
                ).start()
                pl.when(self.inside(self.plane + step))(send)
        self.spread(unit, self.plane, True)

    def four(self, unit, plane, slot, step):
        for pair in range(4):
            block = (pair, plane, self.core)
            self.copy(unit, block, slot, 4 * self.planes + plane, self.ahead(step)).start()

    def along(self, unit, distance):
        z_last = self.units[unit]["z_last"]
        for step in (-1, 1):
            origin = self.plane - step * distance
            onward = self.inside(self.plane + step)

            def take(origin=origin, step=step, onward=onward):
                if z_last:
                    self.wait_blocks(unit, 4, self.recv_sem.at[unit, 4 * self.planes + origin])
                    pl.when(onward)(lambda: self.four(unit, origin, 2 + origin, step))
                    for pair in range(4):
                        self.to_core(unit, (pair, origin, self.core))
                    return
                self.arrived(unit, self.pair, origin)
                block = (self.pair, origin, self.core)
                send = lambda: self.copy(
                    unit, block, 2 + origin, self.arrival(block), self.ahead(step)
                ).start()
                pl.when(onward)(send)
                self.spread(unit, origin)

            pl.when(self.inside(origin))(take)

    def planes_here(self, unit):
        return (self.plane,) if self.units[unit]["z_last"] else range(self.planes)

    def from_near(self, unit):
        near, far, _ = self.partners(unit)
        for plane in self.planes_here(unit):
            self.arrived(unit, near, plane)
            self.share(unit, (near, plane, self.core), far)
            self.to_core(unit, (near, plane, self.core))

    def from_far(self, unit):
        _, far, both = self.partners(unit)
        for pair in (far, both):
            for plane in self.planes_here(unit):
                self.arrived(unit, pair, plane)
                self.to_core(unit, (pair, plane, self.core))
        if self.units[unit]["z_last"]:
            self.keep_own(unit)
            for up in (0, 1):
                step = 2 * up - 1
                pl.when(self.inside(self.plane + step))(
                    lambda up=up, step=step: self.four(unit, self.plane, up, step)
                )

    def keep(self, unit):
        here = (self.pair, self.plane, self.core)
        source, place = self.units[unit]["own"], self.units[unit]["place"](*here)
        return pltpu.make_async_copy(source, place, self.units[unit]["keep_sem"])

    def keep_own(self, unit):
        self.keep(unit).wait()

    def from_core(self, unit):
        if not self.units[unit]["z_last"]:
            self.keep_own(unit)
        self.wait_blocks(unit, 4 * self.planes, self.recv_sem.at[unit, 5 * self.planes])

    def drain(self, unit):
        z_last = self.units[unit]["z_last"]
        along = 4 if z_last else 1

        def sent(slot):
            self.wait_blocks(unit, along, self.send_sem.at[unit, slot])

        for up in (0, 1):
            step = 2 * up - 1
            ahead = self.inside(self.plane + step)
            pl.when(ahead)(lambda up=up: sent(up))
            for distance in range(1, self.planes):
                origin = self.plane - step * distance
                pl.when(ahead & self.inside(origin))(lambda origin=origin: sent(2 + origin))
        shared = 3 + 4 * self.planes if z_last else 7 * self.planes
        self.wait_blocks(unit, shared, self.send_sem.at[unit, 2 + self.planes])


class Scatter(Route):
    @staticmethod
    def send_slots(planes):
        return 3 + 3 * planes

    @staticmethod
    def arrival_slots(planes):
        return 6 + 3 * planes

    @staticmethod
    def buffers(planes, block, z_first):
        shapes = [(4, planes), (2, planes), (planes,), (2, planes)]
        if z_first:
            shapes = [(4, planes), (2, 1), (1,), (2, planes, 4)]
        return [pltpu.VMEM((*shape, *block), BF16) for shape in shapes]

    def core_copy(self, unit, pair, plane):
        source = self.units[unit]["place"](pair, plane, 1 - self.core)
        target = self.units[unit]["core"].at[pair, plane]
        other = (self.pair, self.plane, 1 - self.core)
        return self.remote(source, target, unit, 0, pair, other)

    def far_copy(self, unit, which, pair):
        held = self.units[unit]
        _, far, _ = self.partners(unit)
        target = (far, self.plane, self.core)
        source = held["core"].at[pair]
        if held["z_first"]:
            source = source.at[pl.ds(self.plane, 1)]
        return self.remote(source, held["far"].at[which], unit, 1 + which, 4 + which, target)

    def near_copy(self, unit, plane):
        held = self.units[unit]
        near, _, _ = self.partners(unit)
        target = (near, self.plane, self.core)
        source, place = held["far"].at[1, plane], held["near"].at[plane]
        return self.remote(source, place, unit, 3 + plane, 6 + plane, target)

    def z_copy(self, unit, up, plane, first):
        held = self.units[unit]
        source = held["z"].at[up, plane]
        if first:
            source = held["core"].at[:, plane] if held["z_first"] else held["near"].at[plane]
        target = (self.pair, self.plane + 2 * up - 1, self.core)
        line = (1 + up) * self.planes + plane
        return self.remote(source, held["z"].at[up, plane], unit, 3 + line, 6 + line, target)

    def launch(self, unit, pair, planes=None):
        for plane in range(self.planes) if planes is None else planes:
            self.core_copy(unit, pair, plane).start()

    def add(self, target, term):
        target[...] = (target[...].astype(F32) + term[...].astype(F32)).astype(target.dtype)

    def add_each(self, count, target_of, term_of):
        loop(count, lambda i: self.add(target_of(i), term_of(i)))

    def from_core(self, unit, turn):
        held = self.units[unit]
        pair = self.turn(turn)
        arrived = held["core"].at[pair]
        pltpu.make_async_copy(arrived, arrived, self.recv_sem.at[unit, pair]).wait()
        self.add_each(
            self.planes, lambda i: arrived.at[i], lambda i: held["place"](pair, i, self.core)
        )
        if held["z_first"]:
            if turn == 3:
                self.start_z(unit, range(self.planes))
        elif turn == 0:
            self.far_copy(unit, 1, pair).start()
        elif turn == (1 if held["order"] == 0 else 2):
            self.far_copy(unit, 0, pair).start()

    def from_far(self, unit):
        held = self.units[unit]
        near, far, both = self.partners(unit)
        mine = (lambda pair, i: held["core"].at[pair, self.plane]) if held["z_first"] else (
            lambda pair, i: held["core"].at[pair, i]
        )
        count = held["near"].shape[0]
        self.far_copy(unit, 1, both).wait_recv()
        for plane in self.ends_first(count):
            self.add(held["far"].at[1, plane], mine(near, plane))
            self.near_copy(unit, plane).start()
        self.far_copy(unit, 0, far).wait_recv()
        self.add_each(count, lambda i: held["far"].at[0, i], lambda i: mine(self.pair, i))

    def ends_first(self, count):
        return sorted(range(count), key=lambda plane: min(plane, count - 1 - plane))

    def z_cases(self, up):
        step = 2 * up - 1
        starts = jnp.logical_not(self.inside(self.plane - step))
        for distance in range(self.planes - 1, 0, -1):
            target = self.plane + step * distance
            inside = self.inside(target)
            yield target, inside & starts, inside & jnp.logical_not(starts)

    def start_z(self, unit, planes):
        for target in planes:
            for up, end, ahead in ((1, 0, target > 0), (0, self.planes - 1, target < self.planes - 1)):
                if ahead:
                    pl.when(self.plane == end)(
                        lambda up=up, target=target: self.z_copy(unit, up, target, True).start()
                    )

    def from_near(self, unit):
        held = self.units[unit]
        for plane in self.ends_first(held["near"].shape[0]):
            self.near_copy(unit, plane).wait_recv()
            self.add(held["near"].at[plane], held["far"].at[0, plane])
            if not held["z_first"]:
                self.start_z(unit, (plane,))
        if held["z_first"]:
            held["result"][...] = held["near"][0].astype(F32)

    def from_z(self, unit, hop):
        for up in (0, 1):
            come = self.plane if up else self.planes - 1 - self.plane
            step = 2 * up - 1

            def go(up=up, step=step):
                for distance in range(self.planes - 1 - hop, 0, -1):
                    self.z_pass(unit, up, self.plane + step * distance)

            pl.when(come == hop)(go)

    def z_pass(self, unit, up, target):
        held = self.units[unit]
        self.z_copy(unit, up, target, False).wait_recv()
        place = held["z"].at[up, target]
        if held["z_first"]:
            self.add_each(4, lambda i: place.at[i], lambda i: held["core"].at[i, target])
        else:
            self.add(place, held["near"].at[target])
        self.z_copy(unit, up, target, False).start()

    def finish(self, unit):
        held = self.units[unit]
        z_first = held["z_first"]
        if not z_first:
            held["result"][...] = held["near"][self.plane].astype(F32)
        for up in (0, 1):

            def take(up=up):
                self.z_copy(unit, up, self.plane, False).wait_recv()
                if z_first:
                    self.add_each(
                        4,
                        lambda i: held["core"].at[i, self.plane],
                        lambda i: held["z"].at[up, self.plane, i],
                    )
                else:
                    held["result"][...] += held["z"][up, self.plane].astype(F32)

            pl.when(self.inside(self.plane - 2 * up + 1))(take)
        if z_first:
            _, far, both = self.partners(unit)
            self.far_copy(unit, 1, both).start()
            self.far_copy(unit, 0, far).start()

    def drain(self, unit):
        _, far, both = self.partners(unit)
        core = self.units[unit]["core"]
        pltpu.make_async_copy(core, core, self.send_sem.at[unit, 0]).wait()
        self.far_copy(unit, 1, both).wait_send()
        self.far_copy(unit, 0, far).wait_send()
        for plane in range(self.units[unit]["near"].shape[0]):
            self.near_copy(unit, plane).wait_send()
        for up in (0, 1):
            for target, starts, passes in self.z_cases(up):
                pl.when(starts | passes)(
                    lambda up=up, target=target: self.z_copy(unit, up, target, False).wait_send()
                )


def norm_rows(widths):
    return [-(-width // 128) for width in widths]


def unpack_first(small, part, weight, wide):
    def body(owner):
        rows = pl.ds(pl.multiple_of(owner * part, part), part)
        wide[0, rows, :] = small[owner].astype(F32)[:part]

    loop(small.shape[0], body)
    weight[...] = wide[0].astype(BF16)


def norm_places(norms, lane_rows):
    row = 0
    for norm, rows in zip(norms, lane_rows):
        for i in range(4):
            for j in range(rows):
                lanes = min(128, norm.shape[1] - 128 * j)
                yield row, lanes, norm, i, 128 * j
                row += 1


def unpack_second(small, part, lane_rows, weights, wide, norms, norm_sum):
    norm_sum[...] = jnp.zeros_like(norm_sum)

    def body(owner):
        block = small[owner].astype(F32)
        rows = pl.ds(pl.multiple_of(owner * part, part), part)
        wide[1, rows, :] = block[:part]
        wide[2, rows, :] = block[part : 2 * part]
        norm_sum[...] += block[2 * part : 2 * part + norm_sum.shape[0]]

    loop(small.shape[0], body)
    for i, weight in enumerate(weights):
        weight[...] = wide[1 + i].astype(BF16)
    for row, lanes, norm, i, lane in norm_places(norms, lane_rows):
        norm[i : i + 1, lane : lane + lanes] = norm_sum[row : row + 1, :lanes]


def padded(pieces, rows):
    tail = rows - sum(piece.shape[0] for piece in pieces)
    if tail:
        pieces = [*pieces, jnp.zeros((tail, pieces[0].shape[1]), F32)]
    return jnp.concatenate(pieces, axis=0).astype(BF16)


def pack_first(small, part, wide):
    def body(owner):
        rows = pl.ds(pl.multiple_of(owner * part, part), part)
        small[owner] = padded([wide[0, rows, :]], small.shape[1])

    loop(small.shape[0], body)


def pack_second(small, part, lane_rows, wide, norms, norm_sum):
    norm_sum[...] = jnp.zeros_like(norm_sum)
    for row, lanes, norm, i, lane in norm_places(norms, lane_rows):
        norm_sum[row : row + 1, :lanes] = norm[i : i + 1, lane : lane + lanes]

    def body(owner):
        rows = pl.ds(pl.multiple_of(owner * part, part), part)
        pieces = [wide[1, rows, :], wide[2, rows, :], norm_sum[...]]
        small[owner] = padded(pieces, small.shape[1])

    loop(small.shape[0], body)


def due(plan, engine, slot):
    return [
        functools.partial(getattr(engine, step), *args) for at_slot, step, *args in plan if at_slot == slot
    ]


def move_on(plan, engine, slot):
    for task in due(plan, engine, slot):
        task()


def move_on_at(plan, engine, first, count, index):
    for i in range(count):
        tasks = due(plan, engine, first + i)

        def run(tasks=tasks):
            for task in tasks:
                task()

        if tasks:
            pl.when(index == i)(run)


def whole_kernel(planes, dims, scales, chunks, part, lpart, *refs):
    (
        lengths, x, yt, gx, gyt, own, own_first, own_second,
        text_out, layout_out, dx, dyt, gown_attn, gown_up, gown_down, gown_first, gown_second,
        y, gy, attn, up, down, small_first, small_second, lattn, lup, ldown, wide, norm_sum,
        tnorm, lnorm, gtnorm, glnorm,
        qkv_t, qkv_l, ctx_tt, ctx_tl, ctx_t, ctx_l, act_t, act_l, slope_t, slope_l,
        dhid_t, dhid_l, hat_t, hat_l, low_t, low_l, dlow_t, dlow_l, rate_t, rate_l, lse,
        *held,
    ) = refs
    local_sem, gsend, grecv, ssend, srecv = held[-5:]
    widths = (x.shape[1], y.shape[1])
    lane_rows = norm_rows(widths)
    length = lengths[0]
    half_rows = part // 2

    def owner_of(pair, plane, core):
        return (pair * planes + plane) * 2 + core

    def text_unit(whole, first, rows, order, z_apart):
        def place(pair, plane, core):
            row = owner_of(pair, plane, core) * part + first
            return whole.at[pl.ds(pl.multiple_of(row, 16), rows), :]

        return {
            "place": place,
            "sized": lambda count: whole.at[pl.ds(0, count * rows), :],
            "order": order,
            "z_last": z_apart,
            "z_first": z_apart,
        }

    def small_unit(whole, order, z_apart):
        return {
            "place": lambda *block: whole.at[owner_of(*block)],
            "sized": lambda count: whole.at[pl.ds(0, count)],
            "order": order,
            "z_last": z_apart,
            "z_first": z_apart,
        }

    gunits, sunits = [], []
    texts = ((attn, gown_attn), (up, gown_up), (down, gown_down))
    for which, first, rows, *way in text_cuts(part):
        unit = text_unit(texts[which][0], first, rows, *way)
        gunits.append({"own": own.at[which, pl.ds(first, rows), :], **unit})
        sunits.append({"result": texts[which][1].at[pl.ds(first, rows), :], **unit})
    for whole, source, result, way in (
        (small_first, own_first, gown_first, (0, False)),
        (small_second, own_second, gown_second, (1, SECOND_APART)),
    ):
        gunits.append({"own": source, **small_unit(whole, *way)})
        sunits.append({"result": result, **small_unit(whole, *way)})
    for i, unit in enumerate(sunits):
        unit.update(zip(("core", "far", "near", "z"), held[4 * i : 4 * i + 4]))
    for i, unit in enumerate(gunits):
        unit["keep_sem"] = local_sem.at[i]
    ATTN, UP, DOWN, FIRST, SECOND = (0, 1), (2, 3), (4, 5), (6,), (7,)

    entry_barrier(planes)
    gather = Gather(planes, gunits, gsend, grecv)
    scatter = Scatter(planes, sunits, ssend, srecv)
    def every(step, units, *args):
        for unit in units:
            step(unit, *args)

    def forth(slot):
        move_on(GATHER_PLAN, gather, slot)

    def back(slot):
        move_on(SCATTER_PLAN, scatter, slot)

    start = (*ATTN, *FIRST)
    every(gather.launch, start)
    for unit in range(len(gunits)):
        gather.keep(unit).start()
    y[...] = yt[...].T
    gy[...] = gyt[...].T
    for distance in range(1, planes):
        every(gather.along, start, distance)
    every(gather.from_near, start)
    forth(0)
    every(gather.from_far, start)
    forth(1)
    every(gather.from_core, start)
    forth(2)
    unpack_first(small_first, lpart, lattn, wide)
    project_heads(y, lattn, qkv_l, scales[1], chunks[1])
    forth(3)
    project_heads(x, attn, qkv_t, scales[0], chunks[0])

    def attend(head):
        move_on_at(GATHER_PLAN, gather, 4, HEADS, head)
        attend_head(head, length, qkv_t, qkv_l, ctx_tt, ctx_tl, lse, dims, widths)

    loop(HEADS, attend)
    forth(16)
    every(gather.from_core, SECOND)
    unpack_second(small_second, lpart, lane_rows, (lup, ldown), wide, (tnorm, lnorm), norm_sum)
    nothing = lambda i, block: None
    stream_first(x, ctx_tt, ctx_t, attn, tnorm, dhid_t, hat_t, rate_t, low_t)
    forth(17)
    stream_first(y, ctx_tl, ctx_l, lattn, lnorm, dhid_l, hat_l, rate_l, low_l)
    forth(18)
    stream_up(low_l, lup, act_l, slope_l, chunks[1])
    forth(19)
    every(gather.from_core, UP)
    stream_up(low_t, up, act_t, slope_t, chunks[0])
    forth(20)
    stream_down(act_l, ldown, dhid_l, chunks[1])
    stream_second(gy, lnorm, dhid_l, hat_l, gy, dhid_l, dlow_l, glnorm)
    layout_out[...] = gy[...].T
    forth(21)
    every(gather.from_core, DOWN)
    stream_down(act_t, down, dhid_t, chunks[0])
    stream_second(gx, tnorm, dhid_t, hat_t, text_out, dhid_t, dlow_t, gtnorm)
    every(gather.drain, range(len(gunits)))

    by_chunk = chunks[0] // (2 * part)
    by_pair = planes // by_chunk
    pair_chunks = 4 * by_pair
    inner_units = (*UP, *DOWN)

    def chunk_of(i):
        return scatter.turn(i // by_pair) * by_pair + lax.rem(i, by_pair)

    def planes_of(i):
        return [lax.rem(i, by_pair) * by_chunk + j for j in range(by_chunk)]

    def inner_ready(i, block):
        every(scatter.launch, inner_units, scatter.turn(i // by_pair), planes_of(i))
        move_on_at(SCATTER_PLAN, scatter, 0, pair_chunks, i)

    stream_inner_back(
        low_t, dlow_t, up, down, act_t, slope_t, dhid_t, up, down, chunks[0], inner_ready, chunk_of
    )
    back(8)
    stream_inner_back(
        low_l, dlow_l, lup, ldown, act_l, slope_l, dhid_l, wide.at[1], wide.at[2], chunks[1], nothing
    )
    back(9)
    stream_first_back(
        lnorm, hat_l, rate_l, dhid_l, dlow_l, ctx_l, lattn, ctx_tl, wide.at[0], glnorm
    )
    back(10)
    stream_first_back(tnorm, hat_t, rate_t, dhid_t, dlow_t, ctx_t, attn, ctx_tt, attn, gtnorm)
    every(scatter.launch, ATTN, 3)
    pack_second(small_second, lpart, lane_rows, wide, (gtnorm, glnorm), norm_sum)
    for pair in range(4):
        every(scatter.launch, SECOND, pair)
    back(11)

    def attend_back(head):
        move_on_at(SCATTER_PLAN, scatter, 12, HEADS, head)
        attend_head_back(
            head, length, qkv_t, qkv_l, ctx_tt, ctx_tl, lse, qkv_t, qkv_l, dims, widths, scales
        )

    loop(HEADS, attend_back)
    back(24)
    project_back(y, lattn, qkv_l, dhid_l, y, wide.at[0], chunks[1], nothing)
    dyt[...] = y[...].T
    pack_first(small_first, lpart, wide)
    for pair in range(4):
        every(scatter.launch, FIRST, pair)
    back(25)

    def attn_ready(i, block):
        every(scatter.launch, ATTN, i // by_pair, planes_of(i))
        move_on_at(SCATTER_PLAN, scatter, 26, 3 * by_pair, i)

    project_back(x, attn, qkv_t, dhid_t, dx, attn, chunks[0], attn_ready)
    back(32)
    every(scatter.drain, range(len(sunits)))


def text_cuts(part):
    half = part // 2
    return (
        (0, 0, half, 0, False),
        (0, half, half, 1, False),
        (1, 0, half, 0, False),
        (1, half, half, 1, False),
        (2, 0, half, 0, False),
        (2, half, half, 1, False),
    )


def whole_layer(planes, x, yt, lengths, gx, gyt, own, own_first, own_second, lpart, linner):
    rows, width = x.shape
    lwidth = yt.shape[0]
    owners = 4 * planes * 2
    part = own.shape[1]
    inner = owners * part
    dims = (width // HEADS, lwidth // HEADS)
    scales = tuple(float(dim) ** -0.5 for dim in dims)
    vmem = pl.BlockSpec(memory_space=pltpu.VMEM)
    anywhere = pl.BlockSpec(memory_space=pl.ANY)
    smem = pl.BlockSpec(memory_space=pltpu.SMEM)
    like = jax.ShapeDtypeStruct
    norm_count = 4 * sum(norm_rows((width, lwidth)))

    def both(shape_of, dtype):
        return [pltpu.VMEM(shape_of(width, inner), dtype), pltpu.VMEM(shape_of(lwidth, linner), dtype)]

    held = []
    for _, _, cut, _, z_apart in text_cuts(part):
        held += Scatter.buffers(planes, (cut, width), z_apart)
    for own_small, z_apart in ((own_first, False), (own_second, SECOND_APART)):
        held += Scatter.buffers(planes, own_small.shape, z_apart)
    units = len(held) // 4
    scratch = [
        pltpu.VMEM((rows, lwidth), BF16),
        pltpu.VMEM((rows, lwidth), BF16),
        pltpu.VMEM((inner, width), BF16),
        pltpu.VMEM((inner, width), BF16),
        pltpu.VMEM((inner, width), BF16),
        pltpu.VMEM((owners, *own_first.shape), BF16),
        pltpu.VMEM((owners, *own_second.shape), BF16),
        pltpu.VMEM((linner, lwidth), BF16),
        pltpu.VMEM((linner, lwidth), BF16),
        pltpu.VMEM((linner, lwidth), BF16),
        pltpu.VMEM((3, linner, lwidth), F32),
        pltpu.VMEM((norm_count, lwidth), F32),
        *both(lambda w, f: (4, w), F32),
        *both(lambda w, f: (4, w), F32),
        *both(lambda w, f: (3 * w, rows), BF16),
        *both(lambda w, f: (w, rows), BF16),
        *both(lambda w, f: (rows, w), BF16),
        *both(lambda w, f: (f, rows), BF16),
        *both(lambda w, f: (f, rows), BF16),
        *both(lambda w, f: (rows, w), F32),
        *both(lambda w, f: (rows, w), F32),
        *both(lambda w, f: (rows, w), BF16),
        *both(lambda w, f: (rows, w), BF16),
        *both(lambda w, f: (rows, 1), F32),
        pltpu.VMEM((HEADS, 1, rows), F32),
        *held,
        pltpu.SemaphoreType.DMA((units,)),
        pltpu.SemaphoreType.DMA((units, Gather.send_slots(planes))),
        pltpu.SemaphoreType.DMA((units, Gather.arrival_slots(planes))),
        pltpu.SemaphoreType.DMA((units, Scatter.send_slots(planes))),
        pltpu.SemaphoreType.DMA((units, Scatter.arrival_slots(planes))),
    ]
    return pl.pallas_call(
        functools.partial(whole_kernel, planes, dims, scales, (384, 192), part, lpart),
        out_shape=[
            like(x.shape, BF16),
            like(yt.shape, BF16),
            like(x.shape, BF16),
            like(yt.shape, BF16),
            *[like(own.shape[1:], F32)] * 3,
            like(own_first.shape, F32),
            like(own_second.shape, F32),
        ],
        in_specs=[smem] + [vmem] * 4 + [anywhere] * 3,
        out_specs=[vmem] * 9,
        scratch_shapes=scratch,
        compiler_params=pltpu.CompilerParams(
            collective_id=0, has_side_effects=True, vmem_limit_bytes=67043328
        ),
        name="whole_layer",
    )(lengths, x, yt, gx, gyt, own, own_first, own_second)


def results_kernel(cuts, *refs):
    count = len(cuts)
    sources, rest = refs[: -2 * count - 2], refs[-2 * count - 2 :]
    targets, held, (in_sem, out_sem) = rest[:count], rest[count : 2 * count], rest[2 * count :]
    takes, puts = [], []
    for i, (which, rows, lanes) in enumerate(cuts):
        source = sources[which].at[pl.ds(*rows), pl.ds(0, lanes)]
        takes.append(pltpu.make_async_copy(source, held[i], in_sem.at[i]))
        puts.append(pltpu.make_async_copy(held[i], targets[i], out_sem.at[i]))
        takes[i].start()
    for take, put in zip(takes, puts):
        take.wait()
        put.start()
    for put in puts:
        put.wait()


def results(arrays, cuts):
    shapes = [((rows[1], lanes), arrays[which].dtype) for which, rows, lanes in cuts]
    anywhere = pl.BlockSpec(memory_space=pl.ANY)
    return pl.pallas_call(
        functools.partial(results_kernel, cuts),
        out_shape=[jax.ShapeDtypeStruct(*shape) for shape in shapes],
        in_specs=[anywhere] * len(arrays),
        out_specs=[anywhere] * len(cuts),
        scratch_shapes=[pltpu.VMEM(*shape) for shape in shapes]
        + [pltpu.SemaphoreType.DMA((len(cuts),))] * 2,
        name="results",
    )(*arrays)


def pack_small(pieces, norm_part, multiple):
    owners, _, width = pieces[0].shape
    norm_part = jnp.pad(norm_part, ((0, 0), (0, -norm_part.shape[1] % width)))
    block = jnp.concatenate([*pieces, norm_part.reshape(owners, -1, width)], axis=1)
    return jnp.pad(block, ((0, 0), (0, -block.shape[1] % multiple), (0, 0)))


def unpack_small(block, part, count):
    pieces = [block[:, i * part : (i + 1) * part] for i in range(3)]
    return pieces, block[:, 3 * part :].reshape(block.shape[0], -1)[:, :count]


def lanes_of(flat, widths):
    pieces, first = [], 0
    for width in widths:
        piece = flat[first : first + 4 * width].reshape(4, width)
        first += 4 * width
        pieces.append(jnp.pad(piece, ((0, 0), (0, -width % 128))).reshape(-1, 128))
    return jnp.concatenate(pieces, axis=0)


def flat_of(lanes, widths):
    pieces, first = [], 0
    for width, rows in zip(widths, norm_rows(widths)):
        piece = lanes[first : first + 4 * rows].reshape(4, rows * 128)
        first += 4 * rows
        pieces.append(piece[:, :width].reshape(-1))
    return jnp.concatenate(pieces)


def by_kernel(
    planes, text_in, layout_in, lengths, attn_text, up_text, down_text,
    attn_layout, up_layout, down_layout, norm_params, grad_text, grad_layout,
):
    width, lwidth = text_in.shape[1], layout_in.shape[1]
    owners = lax.axis_size(AXES)
    text_part, part = down_text.shape[0], down_layout.shape[0]
    count = norm_params.shape[0]
    own = jnp.stack([attn_text.T, up_text.T, down_text])
    first = lax.axis_index(AXES) * count
    spread = jnp.pad(norm_params, ((owners - 1) * count, (owners - 1) * count))
    spread = lax.dynamic_slice(spread, ((owners - 1) * count - first,), (owners * count,))
    lanes = lanes_of(spread, (width, lwidth))
    lanes = jnp.pad(lanes, ((0, 0), (0, lwidth - 128)))
    own_first, own_second = (
        jnp.pad(block, ((0, -block.shape[0] % 16), (0, 0)))
        for block in (attn_layout.T, jnp.concatenate([up_layout.T, down_layout, lanes], axis=0))
    )
    arrays = whole_layer(
        planes, text_in, layout_in.T, lengths, grad_text, grad_layout.T, own, own_first, own_second,
        part, owners * part,
    )
    cuts = [(i, (0, array.shape[0]), array.shape[1]) for i, array in enumerate(arrays[:7])]
    cuts += [(7, (0, part), lwidth), (8, (0, part), lwidth), (8, (part, part), lwidth)]
    cuts += [(8, (2 * part, lanes.shape[0]), 128)]
    text_out, layout_out, dx, dy, gattn, gup, gdown, glattn, glup, gldown, gnorm = results(
        arrays, cuts
    )
    gnorm = lax.dynamic_slice(flat_of(gnorm, (width, lwidth)), (first,), (count,))
    return (
        text_out, layout_out.T, dx, dy.T, gattn.T, gup.T, gdown, glattn.T, glup.T, gldown, gnorm,
    )


def by_collectives(
    text_in, layout_in, lengths, attn_text, up_text, down_text,
    attn_layout, up_layout, down_layout, norm_params, grad_text, grad_layout,
):
    width, lwidth = text_in.shape[1], layout_in.shape[1]
    owners = lax.axis_size(AXES)
    part, count = down_layout.shape[0], norm_params.shape[0]

    def gather(piece):
        return lax.all_gather(piece, AXES, axis=0, tiled=True)

    def scatter(piece):
        return lax.psum_scatter(piece, AXES, scatter_dimension=0, tiled=True)

    small = pack_small(
        [attn_layout.T[None], up_layout.T[None], down_layout[None]], norm_params[None], 16
    )
    pieces, norms = unpack_small(gather(small), part, count)
    lattn, lup, ldown = (piece.reshape(owners * part, lwidth) for piece in pieces)
    norms = norms.reshape(-1).astype(F32)
    tnorm = norms[: 4 * width].reshape(4, width)
    lnorm = norms[4 * width :].reshape(4, lwidth)
    attn, up, down = gather(attn_text.T), gather(up_text.T), gather(down_text)
    (
        text_out, layout_out, dx, dy, gattn, gup, gdown, glattn, glup, gldown, gtnorm, glnorm,
    ) = layer(
        text_in, layout_in, lengths, grad_text, grad_layout, tnorm, lnorm,
        attn, up, down, lattn, lup, ldown,
    )
    gnorm = jnp.concatenate([gtnorm.reshape(-1), glnorm.reshape(-1)]).reshape(owners, count)
    gsmall = pack_small(
        [piece.reshape(owners, part, lwidth) for piece in (glattn, glup, gldown)], gnorm, 16
    )
    gattn, gup, gdown, gsmall = (
        scatter(grad).astype(F32) for grad in (gattn, gup, gdown, gsmall)
    )
    (glattn, glup, gldown), gnorm = unpack_small(gsmall, part, count)
    return (
        text_out, layout_out, dx, dy, gattn.T, gup.T, gdown,
        glattn[0].T, glup[0].T, gldown[0], gnorm[0],
    )


def solution(mesh):
    pairs, columns_on_axis = mesh.shape["dp"], mesh.shape["fsdp"]
    body = by_collectives
    if pairs == 4 and columns_on_axis == 8:
        body = functools.partial(by_kernel, columns_on_axis // 2)
    rows, columns = P(AXES, None), P(None, AXES)
    split = P(AXES)
    return jax.shard_map(
        body,
        mesh=mesh,
        in_specs=(
            rows, rows, split, columns, columns, rows, columns, columns, rows, split, rows, rows,
        ),
        out_specs=(rows, rows, rows, rows, columns, columns, rows, columns, columns, rows, split),
        check_vma=False,
    )
```
